128 devices in a mesh: part: 1, data: 16 (over z, y), stage: 8 (over x, core).
Axes of the slice: x: 4, y: 4, z: 4, core: 2. Of those that a mesh axis runs over, the one named last changes fastest.
Arguments:
- x_in: bfloat16 [32, 128, 1536], P(('part', 'data'))
- y_tgt: bfloat16 [32, 128, 1536], P(('part', 'data'))
- w_up: bfloat16 [8, 1536, 6144], P('stage')
- w_down: bfloat16 [8, 6144, 1536], P('stage')
- gain: float32 [8, 1536], P('stage')
Outputs:
- output 1: float32 [8, 1536, 6144], P(('part', 'stage'))
- output 2: float32 [8, 6144, 1536], P(('part', 'stage'))
- output 3: float32 [8, 1536], P(('part', 'stage'))
- output 4: float32 [1], P('part')
All inputs are finite; a program needn't handle non-finite values.
Results may differ from the reference program's by a relative error of at most 0.00377391.
Values are sent between devices in bfloat16 or wider.
A program may use at most 1 GiB of HBM per device.

```python
import jax
import jax.numpy as jnp
from jax import lax

MICRO_ALL = 32
TOKENS = 128
D = 1536
FF = 6144
LAYERS = 8
EPS = 1e-6
TOK_TOTAL = MICRO_ALL * TOKENS


def setup_inputs(seed: int = 0, part: int = 0) -> dict:
    base_key = jax.random.key(seed)
    key_up, key_down, key_gain, key_data = jax.random.split(base_key, 4)
    key_x, key_y = jax.random.split(jax.random.fold_in(key_data, part), 2)
    w_up = (jax.random.normal(key_up, (LAYERS, D, FF), jnp.float32) * D ** -0.5).astype(jnp.bfloat16)
    w_down = (jax.random.normal(key_down, (LAYERS, FF, D), jnp.float32) * FF ** -0.5).astype(jnp.bfloat16)
    gain = 1.0 + 0.25 * jax.random.normal(key_gain, (LAYERS, D), jnp.float32)
    x_in = jax.random.normal(key_x, (MICRO_ALL, TOKENS, D), jnp.float32).astype(jnp.bfloat16)
    y_tgt = jax.random.normal(key_y, (MICRO_ALL, TOKENS, D), jnp.float32).astype(jnp.bfloat16)
    return {"x_in": x_in, "y_tgt": y_tgt, "w_up": w_up, "w_down": w_down, "gain": gain}


def layer_fwd(x_rows, w_one, w_two, gain_row):
    x_float = x_rows.astype(jnp.float32)
    inv_rms = lax.rsqrt(jnp.mean(x_float * x_float, axis=-1, keepdims=True) + EPS)
    normed = (x_float * inv_rms * gain_row).astype(jnp.bfloat16)
    pre_act = jnp.dot(normed, w_one, preferred_element_type=jnp.float32)
    hidden = jax.nn.gelu(pre_act).astype(jnp.bfloat16)
    update = jnp.dot(hidden, w_two, preferred_element_type=jnp.float32)
    return (x_float + update).astype(jnp.bfloat16)


def layer_bwd(x_rows, d_out, w_one, w_two, gain_row):
    x_float = x_rows.astype(jnp.float32)
    inv_rms = lax.rsqrt(jnp.mean(x_float * x_float, axis=-1, keepdims=True) + EPS)
    unit_x = x_float * inv_rms
    normed = (unit_x * gain_row).astype(jnp.bfloat16)
    pre_act = jnp.dot(normed, w_one, preferred_element_type=jnp.float32)
    act_full, gelu_back = jax.vjp(jax.nn.gelu, pre_act)
    hidden = act_full.astype(jnp.bfloat16)
    g_two = jnp.dot(hidden.T, d_out, preferred_element_type=jnp.float32)
    d_hidden = jnp.dot(d_out, w_two.T, preferred_element_type=jnp.float32)
    d_pre = gelu_back(d_hidden)[0].astype(jnp.bfloat16)
    g_one = jnp.dot(normed.T, d_pre, preferred_element_type=jnp.float32)
    d_normed = jnp.dot(d_pre, w_one.T, preferred_element_type=jnp.float32)
    g_gain = jnp.sum(d_normed * unit_x, axis=0)
    d_unit = d_normed * gain_row
    d_x = inv_rms * (d_unit - unit_x * jnp.mean(d_unit * unit_x, axis=-1, keepdims=True))
    return (d_out.astype(jnp.float32) + d_x).astype(jnp.bfloat16), g_one, g_two, g_gain


def reference(x_in, y_tgt, w_up, w_down, gain):
    def micro_step(state_in, mb_pair):
        acc_one, acc_two, acc_gain, loss_sum = state_in
        x_now, y_now = mb_pair

        def fwd_body(hidden_x, layer_w):
            w_one, w_two, gain_row = layer_w
            return layer_fwd(hidden_x, w_one, w_two, gain_row), hidden_x

        top_out, saved_x = lax.scan(fwd_body, x_now, (w_up, w_down, gain))
        err_top = top_out.astype(jnp.float32) - y_now.astype(jnp.float32)
        d_top = (err_top / TOK_TOTAL).astype(jnp.bfloat16)

        def bwd_body(d_rows, layer_item):
            x_saved, w_one, w_two, gain_row = layer_item
            d_next, g_one, g_two, g_gain = layer_bwd(x_saved, d_rows, w_one, w_two, gain_row)
            return d_next, (g_one, g_two, g_gain)

        layer_grads = lax.scan(bwd_body, d_top, (saved_x, w_up, w_down, gain), reverse=True)[1]
        new_state = (acc_one + layer_grads[0], acc_two + layer_grads[1], acc_gain + layer_grads[2], loss_sum + jnp.sum(err_top * err_top))
        return new_state, None

    init_state = (jnp.zeros((LAYERS, D, FF), jnp.float32), jnp.zeros((LAYERS, FF, D), jnp.float32), jnp.zeros((LAYERS, D), jnp.float32), jnp.zeros((), jnp.float32))
    final_state = lax.scan(micro_step, init_state, (x_in, y_tgt))[0]
    d_up, d_down, d_gain, loss_sum = final_state
    loss_out = (loss_sum / (TOK_TOTAL * D)).reshape(1)
    return d_up, d_down, d_gain, loss_out
```

```python
import functools
import math

import jax
import jax.numpy as jnp
from jax import lax
from jax.experimental import pallas as pl
from jax.experimental.pallas import tpu as pltpu
from jax.sharding import PartitionSpec as P

EPS = 1e-6
C0 = math.sqrt(2.0 / math.pi)
CUB = 0.044715
f32 = jnp.float32
bf16 = jnp.bfloat16
MESH = pl.DeviceIdType.MESH
ROWS = (((0,), (0,)), ((), ()))
LASTS = (((1,), (1,)), ((), ()))


def gelu_u(a):
    t = jnp.tanh(C0 * (a + CUB * (a * a * a)))
    return a * (0.5 * (1.0 + t))


def gelu_both(a):
    a2 = a * a
    t = jnp.tanh(C0 * (a + CUB * (a2 * a)))
    half = 0.5 * (1.0 + t)
    slope = half + (0.5 * a) * (1.0 - t * t) * (C0 + (3.0 * CUB * C0) * a2)
    return a * half, slope


def inv_rms(x):
    return lax.rsqrt(jnp.mean(x * x, axis=-1, keepdims=True) + EPS)


def chain_call(T, D, FF, ny, nz, n_stage, tok_total, cb, nj):
    cw = FF // nj
    last = n_stage - 1
    h = T // 2
    qr = T // 4
    early = (n_stage * 3) // 8

    def kernel(x_ref, y_ref, g_ref, w1, w2, rg, dhg, wt1, wt2, dg_o, loss_o,
               pbuf, qbuf, a_s, acc, xb, ob, rb, db, dxb, ts1, ts2, lossb, exy, exz, dgacc,
               wsem, tsem1, tsem2, xs, xr, ds, dr_, ls, lr, ags, agr, own, exs, exr):
        data = lax.axis_index("data")
        s = lax.axis_index("stage")
        z = data // ny
        y = lax.rem(data, ny)

        def plane(zz, yy):
            return {"data": lax.rem(zz + nz, nz) * ny + lax.rem(yy + ny, ny)}

        yp, ym = lax.rem(y + 1, ny), lax.rem(y + ny - 1, ny)
        zp, zm = lax.rem(z + 1, nz), lax.rem(z + nz - 1, nz)
        nxt = {"stage": lax.rem(s + 1, n_stage)}
        prv = {"stage": lax.rem(s + n_stage - 1, n_stage)}

        cp = pltpu.make_async_copy(w1, pbuf, wsem.at[0])
        cq = pltpu.make_async_copy(w2, qbuf, wsem.at[1])
        cp.start()
        cq.start()

        bar = pltpu.get_barrier_semaphore()
        for dev in [plane(z, y + k) for k in range(1, ny)] + [plane(z + k, y) for k in range(1, nz)] + [nxt, prv]:
            pl.semaphore_signal(bar, inc=1, device_id=dev, device_id_type=MESH)
        pl.semaphore_wait(bar, ny + nz)

        def rc(src, dst, ssem, rsem, dev):
            return pltpu.make_async_remote_copy(src_ref=src, dst_ref=dst, send_sem=ssem, recv_sem=rsem, device_id=dev, device_id_type=MESH)

        yup, ydn, zup, zdn = plane(z, y + 1), plane(z, y - 1), plane(z + 1, y), plane(z - 1, y)
        r0, r1, r2, r3 = pl.ds(0, h), pl.ds(h, h), pl.ds(0, qr), pl.ds(qr, qr)
        r4, r5 = pl.ds(h, qr), pl.ds(h + qr, qr)

        def ag(t, m, src, dst):
            def c(k, a, b, dev):
                return rc(a, b, ags.at[t, m, k], agr.at[t, m, k], dev)
            me = dst.at[z, y, m]
            s1 = [c(0, src.at[m, r0], me.at[r0], yup), c(1, src.at[m, r0], me.at[r0], ydn),
                  c(2, src.at[m, r1], me.at[r1], zup), c(3, src.at[m, r1], me.at[r1], zdn)]
            fw = [(4, (z, ym, m, r2), yup), (5, (z, yp, m, r3), ydn), (6, (zm, y, m, r4), zup), (7, (zp, y, m, r5), zdn)]
            s2 = [c(k, dst.at[i], dst.at[i], dev) for k, i, dev in fw]
            al = slice(None)
            f3 = [(8, (z, al, m, r0), zup), (9, (z, al, m, r0), zdn), (10, (al, y, m, r1), yup), (11, (al, y, m, r1), ydn)]
            s3 = [c(k, dst.at[i], dst.at[i], dev) for k, i, dev in f3]
            f4 = [(12, (zm, al, m, r2), zup), (13, (zp, al, m, r3), zdn), (14, (al, ym, m, r4), yup), (15, (al, yp, m, r5), ydn)]
            s4 = [c(k, dst.at[i], dst.at[i], dev) for k, i, dev in f4]
            loc = pltpu.make_async_copy(src.at[m], me, own.at[t, m])
            return s1, s2, s3, s4, loc

        def ag_start(t, m, src, dst):
            s1, _, _, _, loc = ag(t, m, src, dst)
            for c in s1:
                c.start()
            loc.start()

        def ag_two(t, m, src, dst):
            s1, s2, _, _, _ = ag(t, m, src, dst)
            for a, b in zip(s1, s2):
                a.wait_recv()
                b.start()

        def ag_three(t, m, src, dst):
            _, s2, s3, _, loc = ag(t, m, src, dst)
            loc.wait()
            for c in s2:
                c.wait_recv()
            for c in s3:
                c.start()

        def ag_four(t, m, src, dst):
            _, _, s3, s4, _ = ag(t, m, src, dst)
            for a, b in zip(s3, s4):
                a.wait_recv()
                b.start()

        def ag_end(t, m, src, dst):
            s1, s2, s3, s4, _ = ag(t, m, src, dst)
            for c in s4:
                c.wait_recv()
            for c in s1 + s2 + s3 + s4:
                c.wait_send()

        def ag_rest(t, src, dst):
            for step in (ag_two, ag_three, ag_four, ag_end):
                step(t, 0, src, dst)
                step(t, 1, src, dst)

        def transposes():
            nb = FF // cb

            def cp1(c, slot):
                return pltpu.make_async_copy(ts1.at[slot], wt1.at[pl.ds(c * cb, cb), :], tsem1.at[slot])

            def cp2(c, slot):
                return pltpu.make_async_copy(ts2.at[slot], wt2.at[:, pl.ds(c * cb, cb)], tsem2.at[slot])

            def body(c, _):
                slot = lax.rem(c, 2)

                @pl.when(c >= 2)
                def _():
                    cp1(c - 2, slot).wait()
                    cp2(c - 2, slot).wait()
                off = pl.multiple_of(c * cb, cb)
                ts1[slot] = pbuf[:, pl.ds(off, cb)].T
                ts2[slot] = qbuf[pl.ds(off, cb), :].T
                cp1(c, slot).start()
                cp2(c, slot).start()
                return 0
            lax.fori_loop(0, nb, body, 0)
            for c in (nb - 2, nb - 1):
                cp1(c, c % 2).wait()
                cp2(c, c % 2).wait()

        gain = g_ref[...]

        def two_dots(first):
            def second(j, u):
                p = jnp.dot(u, qbuf[j * cw:(j + 1) * cw, :], preferred_element_type=f32)
                if j == 0:
                    acc[...] = p
                else:
                    acc[...] += p
            u = first(0)
            for j in range(1, nj):
                un = first(j)
                second(j - 1, u)
                u = un
            second(nj - 1, u)

        @pl.when(s == 0)
        def _():
            xb[...] = x_ref[...]
        lossb[...] = jnp.zeros_like(lossb)
        cp.wait()
        cq.wait()

        @pl.when(s >= early)
        def _():
            transposes()

        def x_send(m):
            return rc(ob.at[m], xb.at[m], xs.at[m], xr.at[m], nxt)

        def fwd(m, _):
            @pl.when(s > 0)
            def _():
                x_send(m).wait_recv()
            x = xb[m].astype(f32)
            r = (x * inv_rms(x) * gain).astype(bf16)
            rb[m] = r
            ag_start(0, m, rb, rg)

            def first(j):
                a = jnp.dot(r, pbuf[:, j * cw:(j + 1) * cw], preferred_element_type=f32)
                a_s[m, :, j * cw:(j + 1) * cw] = a
                return gelu_u(a).astype(bf16)
            two_dots(first)
            ob[m] = (xb[m].astype(f32) + acc[...]).astype(bf16)

            @pl.when(s < last)
            def _():
                x_send(m).start()

            @pl.when(s == last)
            def _():
                e = ob[m].astype(f32) - y_ref[m].astype(f32)
                lossb[...] += jnp.sum(e * e)
                db[m] = (e * (1.0 / tok_total)).astype(bf16)
            return 0
        lax.fori_loop(0, 2, fwd, 0)

        @pl.when(s < early)
        def _():
            transposes()
        bp = pltpu.make_async_copy(wt2, pbuf, wsem.at[0])
        bq = pltpu.make_async_copy(wt1, qbuf, wsem.at[1])
        bp.start()
        bq.start()

        l_send = rc(lossb, lossb, ls, lr, prv)

        @pl.when(s == last)
        def _():
            l_send.start()

        @pl.when(s < n_stage // 2)
        def _():
            ag_rest(0, rb, rg)
        bp.wait()
        bq.wait()

        def d_send(m):
            return rc(dxb.at[m], db.at[m], ds.at[m], dr_.at[m], prv)

        dgacc[...] = jnp.zeros_like(dgacc)

        def bwd(m, _):
            @pl.when(s < last)
            def _():
                d_send(m).wait_recv()
            ag_start(1, m, db, dhg)
            dh = db[m]

            def first(j):
                du = jnp.dot(dh, pbuf[:, j * cw:(j + 1) * cw], preferred_element_type=f32)
                _, slope = gelu_both(a_s[m, :, j * cw:(j + 1) * cw])
                return (du * slope).astype(bf16)
            two_dots(first)
            x = xb[m].astype(f32)
            q = inv_rms(x)
            n = x * q
            dr = acc[...]
            dn = dr * gain
            dx = q * (dn - n * jnp.mean(dn * n, axis=-1, keepdims=True))
            dxb[m] = (db[m].astype(f32) + dx).astype(bf16)

            @pl.when(s > 0)
            def _():
                d_send(m).start()
            dgacc[...] += jnp.sum(dr * n, axis=0, keepdims=True)
            return 0
        lax.fori_loop(0, 2, bwd, 0)

        @pl.when(s < last)
        def _():
            l_send.wait_recv()

            @pl.when(s > 0)
            def _():
                l_send.start()

        exy[y, :, :D] = jnp.broadcast_to(dgacc[...], (8, D))
        exy[y, :, D:] = lossb[...]

        def ex(axis, k):
            buf, i, dev = (exy, y, plane(z, y + k)) if axis == 0 else (exz, z, plane(z + k, y))
            return rc(buf.at[i], buf.at[i], exs.at[axis, k - 1], exr.at[axis, k - 1], dev)
        for k in range(1, ny):
            ex(0, k).start()

        @pl.when(s >= n_stage // 2)
        def _():
            ag_rest(0, rb, rg)
        ag_two(1, 0, db, dhg)
        ag_two(1, 1, db, dhg)
        for k in range(1, ny):
            ex(0, k).wait_recv()
        tot = exy[0]
        for k in range(1, ny):
            tot = tot + exy[k]
        exz[z] = tot
        for k in range(1, nz):
            ex(1, k).start()
        for step in (ag_three, ag_four):
            step(1, 0, db, dhg)
            step(1, 1, db, dhg)
        for k in range(1, nz):
            ex(1, k).wait_recv()
        tot = exz[0]
        for k in range(1, nz):
            tot = tot + exz[k]
        dg_o[...] = tot[0:1, :D]
        loss_o[...] = tot[0:1, D:] * (1.0 / (tok_total * D))
        ag_end(1, 0, db, dhg)
        ag_end(1, 1, db, dhg)
        for axis, n in ((0, ny), (1, nz)):
            for k in range(1, n):
                ex(axis, k).wait_send()

        @pl.when(s < last)
        def _():
            x_send(0).wait_send()
            x_send(1).wait_send()

        @pl.when(s > 0)
        def _():
            d_send(0).wait_send()
            d_send(1).wait_send()
            l_send.wait_send()

    dma = pltpu.SemaphoreType.DMA
    anyspec = pl.BlockSpec(memory_space=pl.ANY)
    vspec = pl.BlockSpec(memory_space=pltpu.VMEM)
    S = jax.ShapeDtypeStruct
    return pl.pallas_call(
        kernel,
        in_specs=[vspec, vspec, vspec, anyspec, anyspec],
        out_specs=[anyspec, anyspec, anyspec, anyspec, vspec, vspec],
        out_shape=[S((nz, ny, 2, T, D), bf16), S((nz, ny, 2, T, D), bf16), S((FF, D), bf16), S((D, FF), bf16),
                   S((1, D), f32), S((1, 128), f32)],
        scratch_shapes=[
            pltpu.VMEM((D, FF), bf16), pltpu.VMEM((FF, D), bf16), pltpu.VMEM((2, T, FF), f32), pltpu.VMEM((T, D), f32),
            pltpu.VMEM((2, T, D), bf16), pltpu.VMEM((2, T, D), bf16), pltpu.VMEM((2, T, D), bf16),
            pltpu.VMEM((2, T, D), bf16), pltpu.VMEM((2, T, D), bf16),
            pltpu.VMEM((2, cb, D), bf16), pltpu.VMEM((2, D, cb), bf16),
            pltpu.VMEM((8, 128), f32), pltpu.VMEM((ny, 8, D + 128), f32), pltpu.VMEM((nz, 8, D + 128), f32),
            pltpu.VMEM((1, D), f32),
            dma((2,)), dma((2,)), dma((2,)), dma((2,)), dma((2,)), dma((2,)), dma((2,)), dma, dma,
            dma((2, 2, 16)), dma((2, 2, 16)), dma((2, 2)), dma((2, 3)), dma((2, 3))],
        compiler_params=pltpu.CompilerParams(collective_id=0, has_side_effects=True, vmem_limit_bytes=60 << 20),
        cost_estimate=pl.CostEstimate(flops=8 * 2 * T * D * FF * 2, bytes_accessed=6 * D * FF * 2, transcendentals=0),
        name="chain",
    )


def grads_call(T, D, FF, nb, tc, nblk, flip):
    nc = T // tc

    def kernel(r_ref, dh_ref, w1_ref, w2_ref, o1_ref, o2_ref, acc1, uda):
        def first(c):
            base = pl.multiple_of(c * tc, tc)
            a = jnp.dot(r_ref[pl.ds(base, tc), :], w1_ref[...], preferred_element_type=f32)
            du = lax.dot_general(dh_ref[pl.ds(base, tc), :], w2_ref[...], LASTS, preferred_element_type=f32)
            u, slope = gelu_both(a)
            slot = lax.rem(c, 2)
            uda[slot, :, :nb] = u.astype(bf16)
            uda[slot, :, nb:] = (du * slope).astype(bf16)

        def second(c, init):
            base = pl.multiple_of(c * tc, tc)
            slot = lax.rem(c, 2)
            p2 = lax.dot_general(uda[slot, :, :nb], dh_ref[pl.ds(base, tc), :], ROWS, preferred_element_type=f32)
            p1 = lax.dot_general(uda[slot, :, nb:], r_ref[pl.ds(base, tc), :], ROWS, preferred_element_type=f32)
            if init:
                o2_ref[...] = p2
                acc1[...] = p1
            else:
                o2_ref[...] += p2
                acc1[...] += p1
        first(0)
        first(1)
        second(0, True)

        def body(c, _):
            first(c)
            second(c - 1, False)
            return 0
        lax.fori_loop(2, nc, body, 0)
        second(nc - 1, False)
        o1_ref[...] = acc1[...] if flip else acc1[...].T

    S = jax.ShapeDtypeStruct
    n1 = nb * nblk
    full = pl.BlockSpec((T, D), lambda i: (0, 0), pipeline_mode=pl.Buffered(1))
    down = pl.BlockSpec((nb, D), lambda i: (i, 0))
    up = pl.BlockSpec((D, nb), lambda i: (0, i))
    return pl.pallas_call(
        kernel,
        grid=(nblk,),
        in_specs=[full, full, up, down],
        out_specs=[down if flip else up, down],
        out_shape=[S((n1, D) if flip else (D, FF), f32), S((n1 if flip else FF, D), f32)],
        scratch_shapes=[pltpu.VMEM((nb, D), f32), pltpu.VMEM((2, tc, 2 * nb), bf16)],
        compiler_params=pltpu.CompilerParams(vmem_limit_bytes=60 << 20),
        cost_estimate=pl.CostEstimate(flops=8 * n1 * T * D, bytes_accessed=4 * T * D + 12 * n1 * D, transcendentals=0),
        name="grads_slice" if flip else "grads_local",
    )


def place_call(D, FF, ns, n_dev):
    base = (FF - ns * n_dev) // ns

    def kernel(g1, g2, u_in, d_in, u_out, d_out):
        u_out[...] = g1[0].T
        d_out[...] = g2[0]

    S = jax.ShapeDtypeStruct
    src = pl.BlockSpec((1, ns, D), lambda i: (i, 0, 0))
    anyspec = pl.BlockSpec(memory_space=pl.ANY)
    return pl.pallas_call(
        kernel,
        grid=(n_dev,),
        in_specs=[src, src, anyspec, anyspec],
        out_specs=[pl.BlockSpec((D, ns), lambda i: (0, base + i)), pl.BlockSpec((ns, D), lambda i: (base + i, 0))],
        out_shape=[S((D, FF), f32), S((FF, D), f32)],
        input_output_aliases={2: 0, 3: 1},
        cost_estimate=pl.CostEstimate(flops=0, bytes_accessed=16 * ns * n_dev * D, transcendentals=0),
        name="place",
    )


def solution(mesh):
    n_stage = mesh.shape["stage"]
    n_data = mesh.shape["data"]
    ny = int(round(n_data ** 0.5))
    nz = n_data // ny
    ns = 128

    def local_step(x_in, y_tgt, w_up, w_down, gain):
        n_micro, T, D = x_in.shape
        FF = w_up.shape[2]
        w1, w2 = w_up[0], w_down[0]
        tok_total = n_data * n_micro * T
        rg, dhg, _, _, dg, loss = chain_call(T, D, FF, ny, nz, n_stage, tok_total, 256, 4)(x_in, y_tgt, gain, w1, w2)
        rg = rg.reshape(tok_total, D)
        dhg = dhg.reshape(tok_total, D)
        n_loc = FF - ns * n_data
        start = n_loc + lax.axis_index("data") * ns
        s1 = lax.dynamic_slice_in_dim(w1, start, ns, 1)
        s2 = lax.dynamic_slice_in_dim(w2, start, ns, 0)
        p1, p2 = grads_call(tok_total, D, FF, ns, 512, 1, True)(rg, dhg, s1, s2)
        g1 = lax.all_gather(p1, "data", axis=0)
        g2 = lax.all_gather(p2, "data", axis=0)
        up, down = grads_call(tok_total, D, FF, 256, 1024, n_loc // 256, False)(rg, dhg, w1, w2)
        up, down = place_call(D, FF, ns, n_data)(g1, g2, up, down)
        return up[None], down[None], dg, loss[0, :1]

    return jax.shard_map(local_step, mesh=mesh, in_specs=(P(("part", "data"), None, None), P(("part", "data"), None, None), P("stage", None, None), P("stage", None, None), P("stage", None)), out_specs=(P(("part", "stage"), None, None), P(("part", "stage"), None, None), P(("part", "stage"), None), P("part")), check_vma=False)
```

```python
import functools
import math

import jax
import jax.numpy as jnp
from jax import lax
from jax.experimental import pallas as pl
from jax.experimental.pallas import tpu as pltpu
from jax.sharding import PartitionSpec as P

EPS = 1e-6
C0 = math.sqrt(2.0 / math.pi)
CUB = 0.044715
f32 = jnp.float32
bf16 = jnp.bfloat16
MESH = pl.DeviceIdType.MESH
ROWS = (((0,), (0,)), ((), ()))
LASTS = (((1,), (1,)), ((), ()))


def gelu_u(a):
    t = jnp.tanh(C0 * (a + CUB * (a * a * a)))
    return a * (0.5 * (1.0 + t))


def gelu_both(a):
    a2 = a * a
    t = jnp.tanh(C0 * (a + CUB * (a2 * a)))
    half = 0.5 * (1.0 + t)
    slope = half + (0.5 * a) * (1.0 - t * t) * (C0 + (3.0 * CUB * C0) * a2)
    return a * half, slope


def inv_rms(x):
    return lax.rsqrt(jnp.mean(x * x, axis=-1, keepdims=True) + EPS)


def chain_call(T, D, FF, ny, nz, n_stage, tok_total, cb, nj):
    cw = FF // nj
    last = n_stage - 1
    h = T // 2
    qr = T // 4
    early = (n_stage * 3) // 8

    def kernel(x_ref, y_ref, g_ref, w1, w2, rg, dhg, wt1, wt2, dg_o, loss_o,
               pbuf, qbuf, a_s, acc, xb, ob, rb, db, dxb, ts1, ts2, lossb, exy, exz, dgacc,
               wsem, tsem1, tsem2, xs, xr, ds, dr_, ls, lr, ags, agr, own, exs, exr):
        data = lax.axis_index("data")
        s = lax.axis_index("stage")
        z = data // ny
        y = lax.rem(data, ny)

        def plane(zz, yy):
            return {"data": lax.rem(zz + nz, nz) * ny + lax.rem(yy + ny, ny)}

        yp, ym = lax.rem(y + 1, ny), lax.rem(y + ny - 1, ny)
        zp, zm = lax.rem(z + 1, nz), lax.rem(z + nz - 1, nz)
        nxt = {"stage": lax.rem(s + 1, n_stage)}
        prv = {"stage": lax.rem(s + n_stage - 1, n_stage)}

        cp = pltpu.make_async_copy(w1, pbuf, wsem.at[0])
        cq = pltpu.make_async_copy(w2, qbuf, wsem.at[1])
        cp.start()
        cq.start()

        bar = pltpu.get_barrier_semaphore()
        for dev in [plane(z, y + k) for k in range(1, ny)] + [plane(z + k, y) for k in range(1, nz)] + [nxt, prv]:
            pl.semaphore_signal(bar, inc=1, device_id=dev, device_id_type=MESH)
        pl.semaphore_wait(bar, ny + nz)

        def rc(src, dst, ssem, rsem, dev):
            return pltpu.make_async_remote_copy(src_ref=src, dst_ref=dst, send_sem=ssem, recv_sem=rsem, device_id=dev, device_id_type=MESH)

        yup, ydn, zup, zdn = plane(z, y + 1), plane(z, y - 1), plane(z + 1, y), plane(z - 1, y)
        r0, r1, r2, r3 = pl.ds(0, h), pl.ds(h, h), pl.ds(0, qr), pl.ds(qr, qr)
        r4, r5 = pl.ds(h, qr), pl.ds(h + qr, qr)

        def ag(t, m, src, dst):
            def c(k, a, b, dev):
                return rc(a, b, ags.at[t, m, k], agr.at[t, m, k], dev)
            me = dst.at[z, y, m]
            s1 = [c(0, src.at[m, r0], me.at[r0], yup), c(1, src.at[m, r0], me.at[r0], ydn),
                  c(2, src.at[m, r1], me.at[r1], zup), c(3, src.at[m, r1], me.at[r1], zdn)]
            fw = [(4, (z, ym, m, r2), yup), (5, (z, yp, m, r3), ydn), (6, (zm, y, m, r4), zup), (7, (zp, y, m, r5), zdn)]
            s2 = [c(k, dst.at[i], dst.at[i], dev) for k, i, dev in fw]
            al = slice(None)
            f3 = [(8, (z, al, m, r0), zup), (9, (z, al, m, r0), zdn), (10, (al, y, m, r1), yup), (11, (al, y, m, r1), ydn)]
            s3 = [c(k, dst.at[i], dst.at[i], dev) for k, i, dev in f3]
            f4 = [(12, (zm, al, m, r2), zup), (13, (zp, al, m, r3), zdn), (14, (al, ym, m, r4), yup), (15, (al, yp, m, r5), ydn)]
            s4 = [c(k, dst.at[i], dst.at[i], dev) for k, i, dev in f4]
            loc = pltpu.make_async_copy(src.at[m], me, own.at[t, m])
            return s1, s2, s3, s4, loc

        def ag_start(t, m, src, dst):
            s1, _, _, _, loc = ag(t, m, src, dst)
            for c in s1:
                c.start()
            loc.start()

        def ag_two(t, m, src, dst):
            s1, s2, _, _, _ = ag(t, m, src, dst)
            for a, b in zip(s1, s2):
                a.wait_recv()
                b.start()

        def ag_three(t, m, src, dst):
            _, s2, s3, _, loc = ag(t, m, src, dst)
            loc.wait()
            for c in s2:
                c.wait_recv()
            for c in s3:
                c.start()

        def ag_four(t, m, src, dst):
            _, _, s3, s4, _ = ag(t, m, src, dst)
            for a, b in zip(s3, s4):
                a.wait_recv()
                b.start()

        def ag_end(t, m, src, dst):
            s1, s2, s3, s4, _ = ag(t, m, src, dst)
            for c in s4:
                c.wait_recv()
            for c in s1 + s2 + s3 + s4:
                c.wait_send()

        def ag_rest(t, src, dst):
            for step in (ag_two, ag_three, ag_four, ag_end):
                step(t, 0, src, dst)
                step(t, 1, src, dst)

        def transposes():
            nb = FF // cb

            def cp1(c, slot):
                return pltpu.make_async_copy(ts1.at[slot], wt1.at[pl.ds(c * cb, cb), :], tsem1.at[slot])

            def cp2(c, slot):
                return pltpu.make_async_copy(ts2.at[slot], wt2.at[:, pl.ds(c * cb, cb)], tsem2.at[slot])

            def body(c, _):
                slot = lax.rem(c, 2)

                @pl.when(c >= 2)
                def _():
                    cp1(c - 2, slot).wait()
                    cp2(c - 2, slot).wait()
                off = pl.multiple_of(c * cb, cb)
                ts1[slot] = pbuf[:, pl.ds(off, cb)].T
                ts2[slot] = qbuf[pl.ds(off, cb), :].T
                cp1(c, slot).start()
                cp2(c, slot).start()
                return 0
            lax.fori_loop(0, nb, body, 0)
            for c in (nb - 2, nb - 1):
                cp1(c, c % 2).wait()
                cp2(c, c % 2).wait()

        gain = g_ref[...]

        def two_dots(first):
            def second(j, u):
                p = jnp.dot(u, qbuf[j * cw:(j + 1) * cw, :], preferred_element_type=f32)
                if j == 0:
                    acc[...] = p
                else:
                    acc[...] += p
            u = first(0)
            for j in range(1, nj):
                un = first(j)
                second(j - 1, u)
                u = un
            second(nj - 1, u)

        @pl.when(s == 0)
        def _():
            xb[...] = x_ref[...]
        lossb[...] = jnp.zeros_like(lossb)
        cp.wait()
        cq.wait()

        @pl.when(s >= early)
        def _():
            transposes()

        def x_send(m):
            return rc(ob.at[m], xb.at[m], xs.at[m], xr.at[m], nxt)

        def fwd(m, _):
            @pl.when(s > 0)
            def _():
                x_send(m).wait_recv()
            x = xb[m].astype(f32)
            r = (x * inv_rms(x) * gain).astype(bf16)
            rb[m] = r
            ag_start(0, m, rb, rg)

            def first(j):
                a = jnp.dot(r, pbuf[:, j * cw:(j + 1) * cw], preferred_element_type=f32)
                a_s[m, :, j * cw:(j + 1) * cw] = a
                return gelu_u(a).astype(bf16)
            two_dots(first)
            ob[m] = (xb[m].astype(f32) + acc[...]).astype(bf16)

            @pl.when(s < last)
            def _():
                x_send(m).start()

            @pl.when(s == last)
            def _():
                e = ob[m].astype(f32) - y_ref[m].astype(f32)
                lossb[...] += jnp.sum(e * e)
                db[m] = (e * (1.0 / tok_total)).astype(bf16)
            return 0
        lax.fori_loop(0, 2, fwd, 0)

        @pl.when(s < early)
        def _():
            transposes()
        bp = pltpu.make_async_copy(wt2, pbuf, wsem.at[0])
        bq = pltpu.make_async_copy(wt1, qbuf, wsem.at[1])
        bp.start()
        bq.start()

        l_send = rc(lossb, lossb, ls, lr, prv)

        @pl.when(s == last)
        def _():
            l_send.start()

        @pl.when(s < n_stage // 2)
        def _():
            ag_rest(0, rb, rg)
        bp.wait()
        bq.wait()

        def d_send(m):
            return rc(dxb.at[m], db.at[m], ds.at[m], dr_.at[m], prv)

        dgacc[...] = jnp.zeros_like(dgacc)

        def bwd(m, _):
            @pl.when(s < last)
            def _():
                d_send(m).wait_recv()
            ag_start(1, m, db, dhg)
            dh = db[m]

            def first(j):
                du = jnp.dot(dh, pbuf[:, j * cw:(j + 1) * cw], preferred_element_type=f32)
                _, slope = gelu_both(a_s[m, :, j * cw:(j + 1) * cw])
                return (du * slope).astype(bf16)
            two_dots(first)
            x = xb[m].astype(f32)
            q = inv_rms(x)
            n = x * q
            dr = acc[...]
            dn = dr * gain
            dx = q * (dn - n * jnp.mean(dn * n, axis=-1, keepdims=True))
            dxb[m] = (db[m].astype(f32) + dx).astype(bf16)

            @pl.when(s > 0)
            def _():
                d_send(m).start()
            dgacc[...] += jnp.sum(dr * n, axis=0, keepdims=True)
            return 0
        lax.fori_loop(0, 2, bwd, 0)

        @pl.when(s < last)
        def _():
            l_send.wait_recv()

            @pl.when(s > 0)
            def _():
                l_send.start()

        exy[y, :, :D] = jnp.broadcast_to(dgacc[...], (8, D))
        exy[y, :, D:] = lossb[...]

        def ex(axis, k):
            buf, i, dev = (exy, y, plane(z, y + k)) if axis == 0 else (exz, z, plane(z + k, y))
            return rc(buf.at[i], buf.at[i], exs.at[axis, k - 1], exr.at[axis, k - 1], dev)
        for k in range(1, ny):
            ex(0, k).start()

        @pl.when(s >= n_stage // 2)
        def _():
            ag_rest(0, rb, rg)
        ag_two(1, 0, db, dhg)
        ag_two(1, 1, db, dhg)
        for k in range(1, ny):
            ex(0, k).wait_recv()
        tot = exy[0]
        for k in range(1, ny):
            tot = tot + exy[k]
        exz[z] = tot
        for k in range(1, nz):
            ex(1, k).start()
        for step in (ag_three, ag_four):
            step(1, 0, db, dhg)
            step(1, 1, db, dhg)
        for k in range(1, nz):
            ex(1, k).wait_recv()
        tot = exz[0]
        for k in range(1, nz):
            tot = tot + exz[k]
        dg_o[...] = tot[0:1, :D]
        loss_o[...] = tot[0:1, D:] * (1.0 / (tok_total * D))
        ag_end(1, 0, db, dhg)
        ag_end(1, 1, db, dhg)
        for axis, n in ((0, ny), (1, nz)):
            for k in range(1, n):
                ex(axis, k).wait_send()

        @pl.when(s < last)
        def _():
            x_send(0).wait_send()
            x_send(1).wait_send()

        @pl.when(s > 0)
        def _():
            d_send(0).wait_send()
            d_send(1).wait_send()
            l_send.wait_send()

    dma = pltpu.SemaphoreType.DMA
    anyspec = pl.BlockSpec(memory_space=pl.ANY)
    vspec = pl.BlockSpec(memory_space=pltpu.VMEM)
    S = jax.ShapeDtypeStruct
    return pl.pallas_call(
        kernel,
        in_specs=[vspec, vspec, vspec, anyspec, anyspec],
        out_specs=[anyspec, anyspec, anyspec, anyspec, vspec, vspec],
        out_shape=[S((nz, ny, 2, T, D), bf16), S((nz, ny, 2, T, D), bf16), S((FF, D), bf16), S((D, FF), bf16),
                   S((1, D), f32), S((1, 128), f32)],
        scratch_shapes=[
            pltpu.VMEM((D, FF), bf16), pltpu.VMEM((FF, D), bf16), pltpu.VMEM((2, T, FF), f32), pltpu.VMEM((T, D), f32),
            pltpu.VMEM((2, T, D), bf16), pltpu.VMEM((2, T, D), bf16), pltpu.VMEM((2, T, D), bf16),
            pltpu.VMEM((2, T, D), bf16), pltpu.VMEM((2, T, D), bf16),
            pltpu.VMEM((2, cb, D), bf16), pltpu.VMEM((2, D, cb), bf16),
            pltpu.VMEM((8, 128), f32), pltpu.VMEM((ny, 8, D + 128), f32), pltpu.VMEM((nz, 8, D + 128), f32),
            pltpu.VMEM((1, D), f32),
            dma((2,)), dma((2,)), dma((2,)), dma((2,)), dma((2,)), dma((2,)), dma((2,)), dma, dma,
            dma((2, 2, 16)), dma((2, 2, 16)), dma((2, 2)), dma((2, 3)), dma((2, 3))],
        compiler_params=pltpu.CompilerParams(collective_id=0, has_side_effects=True, vmem_limit_bytes=60 << 20),
        cost_estimate=pl.CostEstimate(flops=8 * 2 * T * D * FF * 2, bytes_accessed=6 * D * FF * 2, transcendentals=0),
        name="chain",
    )


class Sweep:
    def __init__(self, T, D, nb, tc, sub, nblk, off, refs, w1, w2, out_up, out_down, up_off, down_off):
        self.T, self.D, self.nb, self.tc, self.sub, self.nblk = T, D, nb, tc, sub, nblk
        self.off, self.up_off, self.down_off = off, up_off, down_off
        self.nc = T // tc
        self.w1, self.w2, self.out_up, self.out_down = w1, w2, out_up, out_down
        self.R, self.DH, self.w1b, self.w2b, self.o1, self.o2, self.uda, self.udb, self.wsem, self.osem = refs

    def wcopy(self, b):
        sl = lax.rem(b, 2)
        at = pl.multiple_of(self.off + b * self.nb, self.nb)
        return (pltpu.make_async_copy(self.w1.at[:, pl.ds(at, self.nb)], self.w1b.at[sl], self.wsem.at[0, sl]),
                pltpu.make_async_copy(self.w2.at[pl.ds(at, self.nb), :], self.w2b.at[sl], self.wsem.at[1, sl]))

    def ocopy(self, b):
        sl = lax.rem(b, 2)
        up = pl.multiple_of(self.up_off + b * self.nb, self.nb)
        dn = pl.multiple_of(self.down_off + b * self.nb, self.nb)
        return (pltpu.make_async_copy(self.o1.at[sl], self.out_up.at[:, pl.ds(up, self.nb)], self.osem.at[0, sl]),
                pltpu.make_async_copy(self.o2.at[sl], self.out_down.at[pl.ds(dn, self.nb), :], self.osem.at[1, sl]))

    def prefetch(self):
        for x in self.wcopy(0):
            x.start()

    def pre(self, i):
        b, c = i // self.nc, lax.rem(i, self.nc)

        @pl.when((c == 0) & (b < self.nblk))
        def _():
            for x in self.wcopy(b):
                x.wait()

            @pl.when(b + 1 < self.nblk)
            def _():
                for x in self.wcopy(b + 1):
                    x.start()

    def mid(self, i):
        b, c = i // self.nc, lax.rem(i, self.nc)

        @pl.when((c == 0) & (b >= 2))
        def _():
            for x in self.ocopy(b - 2):
                x.wait()

    def post(self, i):
        b, c = i // self.nc, lax.rem(i, self.nc)

        @pl.when(c == self.nc - 1)
        def _():
            for x in self.ocopy(b):
                x.start()

    def drain(self):
        for b in (self.nblk - 2, self.nblk - 1):
            if b >= 0:
                for x in self.ocopy(b):
                    x.wait()

    def step(self, i, dst, src):
        nb, tc, sub, D = self.nb, self.tc, self.sub, self.D
        c, sl = lax.rem(i, self.nc), lax.rem(i // self.nc, 2)
        j = i - 1
        jc, jl = lax.rem(j, self.nc), lax.rem(j // self.nc, 2)

        def first(k):
            base = pl.multiple_of(c * tc + k * sub, sub)
            a = jnp.dot(self.R[pl.ds(base, sub), :], self.w1b[sl], preferred_element_type=f32)
            du = lax.dot_general(self.DH[pl.ds(base, sub), :], self.w2b[sl], LASTS, preferred_element_type=f32)
            u, slope = gelu_both(a)
            dst[k * sub:(k + 1) * sub, :nb] = u.astype(bf16)
            dst[k * sub:(k + 1) * sub, nb:] = (du * slope).astype(bf16)

        def second(q):
            keep = jc > 0
            base = pl.multiple_of(jc * tc, tc)
            n = slice(q * 256, (q + 1) * 256)
            p2 = lax.dot_general(src[:, :nb], self.DH[pl.ds(base, tc), n], ROWS, preferred_element_type=f32)
            self.o2[jl, :, n] = jnp.where(keep, self.o2[jl, :, n], 0.0) + p2
            p1 = lax.dot_general(self.R[pl.ds(base, tc), n], src[:, nb:], ROWS, preferred_element_type=f32)
            self.o1[jl, n, :] = jnp.where(keep, self.o1[jl, n, :], 0.0) + p1
        q = 0
        for k in range(tc // sub):
            first(k)
            while src is not None and q < ((k + 1) * (D // 256)) // (tc // sub):
                second(q)
                q += 1

    def run(self, loads, between):
        loads(0)
        self.pre(0)
        self.step(0, self.uda, None)

        def one(i, dst, src):
            between(i)

            @pl.when(i < self.nc)
            def _():
                loads(i)
            self.pre(i)
            self.mid(i - 1)
            self.step(i, dst, src)
            self.post(i - 1)

        def body(ii, _):
            one(2 * ii + 1, self.udb, self.uda)
            one(2 * ii + 2, self.uda, self.udb)
            return 0
        lax.fori_loop(0, self.nblk * self.nc // 2, body, 0)


def sweep_scratch(T, D, nb, tc):
    dma = pltpu.SemaphoreType.DMA
    return [pltpu.VMEM((T, D), bf16), pltpu.VMEM((T, D), bf16), pltpu.VMEM((2, D, nb), bf16), pltpu.VMEM((2, nb, D), bf16),
            pltpu.VMEM((2, D, nb), f32), pltpu.VMEM((2, nb, D), f32), pltpu.VMEM((tc, 2 * nb), bf16),
            pltpu.VMEM((tc, 2 * nb), bf16), dma((2, 2)), dma((2, 2))]


def spread_call(T, D, FF, ny, nz, ns, nb, tc, sub, nblk, when):
    nc = T // tc
    n_loc = FF - ns * ny * nz
    h = ns // 2

    def kernel(rg, dhg, w1, w2, wt1, ga, gb, lu, ld, R, DH, w1b, w2b, o1, o2, uda, udb, wsem, osem,
               s1b, s2b, sa, sb, lsem, ssem, loc, snd, rcv):
        data = lax.axis_index("data")
        z = data // ny
        y = lax.rem(data, ny)

        def plane(zz, yy):
            return {"data": lax.rem(zz + nz, nz) * ny + lax.rem(yy + ny, ny)}

        yup, ydn, zup, zdn = plane(z, y + 1), plane(z, y - 1), plane(z + 1, y), plane(z - 1, y)
        yp, ym, y2 = lax.rem(y + 1, ny), lax.rem(y + ny - 1, ny), lax.rem(y + 2, ny)
        zp, zm, z2 = lax.rem(z + 1, nz), lax.rem(z + nz - 1, nz), lax.rem(z + 2, nz)
        start = pl.multiple_of(n_loc + data * ns, 16)
        sw = [pltpu.make_async_copy(wt1.at[pl.ds(start, ns), :], s1b, ssem.at[0]),
              pltpu.make_async_copy(w2.at[pl.ds(start, ns), :], s2b, ssem.at[1])]
        for x in sw:
            x.start()

        def token_copy(c):
            rows = pl.ds(pl.multiple_of(c * tc, tc), tc)
            return (pltpu.make_async_copy(rg.at[rows], R.at[rows], lsem.at[0, c]),
                    pltpu.make_async_copy(dhg.at[rows], DH.at[rows], lsem.at[1, c]))
        for c in range(nc):
            for x in token_copy(c):
                x.start()
        bar = pltpu.get_barrier_semaphore()
        for dev in (yup, ydn, zup, zdn):
            pl.semaphore_signal(bar, inc=1, device_id=dev, device_id_type=MESH)
        pl.semaphore_wait(bar, 4)
        sweep = Sweep(T, D, nb, tc, sub, nblk, 0, (R, DH, w1b, w2b, o1, o2, uda, udb, wsem, osem), w1, w2, lu, ld, 0, 0)
        sweep.prefetch()
        for x in sw:
            x.wait()

        def own(c, _):
            for x in token_copy(c):
                x.wait()
            base = pl.multiple_of(c * tc, tc)
            for k in range(tc // sub):
                at = pl.multiple_of(base + k * sub, sub)
                a = lax.dot_general(R[pl.ds(at, sub), :], s1b[...], LASTS, preferred_element_type=f32)
                du = lax.dot_general(DH[pl.ds(at, sub), :], s2b[...], LASTS, preferred_element_type=f32)
                u, slope = gelu_both(a)
                uda[k * sub:(k + 1) * sub, :ns] = u.astype(bf16)
                udb[k * sub:(k + 1) * sub, :ns] = (du * slope).astype(bf16)
            keep = c > 0
            for q in range(D // 256):
                n = slice(q * 256, (q + 1) * 256)
                p2 = lax.dot_general(uda[:, :ns], DH[pl.ds(base, tc), n], ROWS, preferred_element_type=f32)
                sb[:, n] = jnp.where(keep, sb[:, n], 0.0) + p2
                p1 = lax.dot_general(udb[:, :ns], R[pl.ds(base, tc), n], ROWS, preferred_element_type=f32)
                sa[:, n] = jnp.where(keep, sa[:, n], 0.0) + p1
            return 0
        lax.fori_loop(0, nc, own, 0)

        h0, h1 = pl.ds(0, h), pl.ds(h, h)
        al = pl.ds(0, ns)

        def rc(k, src, dst, dev):
            return pltpu.make_async_remote_copy(src_ref=src, dst_ref=dst, send_sem=snd.at[k], recv_sem=rcv.at[k], device_id=dev, device_id_type=MESH)

        def thru(k, buf, zz, yy, part, dev):
            return (k, buf.at[zz, yy, part], buf.at[zz, yy, part], dev)
        mine_a, mine_b = ga.at[z, y], gb.at[z, y]
        plan = [
            [(0, sa, mine_a, yup), (1, sa, mine_a, ydn), (2, sb, mine_b, zup), (3, sb, mine_b, zdn),
             (4, sa, mine_a, zup), (5, sa, mine_a, zdn), (6, sb, mine_b, yup), (7, sb, mine_b, ydn)],
            [thru(8, ga, z, ym, h0, yup), thru(9, ga, z, yp, h1, ydn), thru(10, gb, zm, y, h0, zup), thru(11, gb, zp, y, h1, zdn),
             thru(12, ga, z, ym, al, zup), thru(13, ga, z, ym, al, zdn), thru(14, ga, z, yp, al, zup), thru(15, ga, z, yp, al, zdn),
             thru(16, gb, zm, y, al, yup), thru(17, gb, zm, y, al, ydn), thru(18, gb, zp, y, al, yup), thru(19, gb, zp, y, al, ydn)],
            [thru(20, ga, zm, y, h0, zup), thru(21, ga, zp, y, h1, zdn), thru(22, gb, z, ym, h0, yup), thru(23, gb, z, yp, h1, ydn)],
            [thru(24, ga, z, y2, al, zup), thru(25, ga, z, y2, al, zdn), thru(26, gb, z2, y, al, yup), thru(27, gb, z2, y, al, ydn)],
            [thru(28, ga, zm, ym, h0, zup), thru(29, ga, zp, ym, h1, zdn), thru(30, ga, zm, yp, h0, zup), thru(31, ga, zp, yp, h1, zdn),
             thru(32, gb, zm, ym, h0, yup), thru(33, gb, zm, yp, h1, ydn), thru(34, gb, zp, ym, h0, yup), thru(35, gb, zp, yp, h1, ydn)],
            [thru(36, ga, zm, y2, h0, zup), thru(37, ga, zp, y2, h1, zdn), thru(38, gb, z2, ym, h0, yup), thru(39, gb, z2, yp, h1, ydn)],
        ]
        flat = {e[0]: e for group in plan for e in group}
        needs = [[], range(0, 4), range(4, 8), range(8, 12), range(12, 20), range(24, 28)]

        def act(g):
            for k in needs[g]:
                rc(*flat[k]).wait_recv()
            for e in plan[g]:
                rc(*e).start()
        act(0)
        keep_a = pltpu.make_async_copy(sa, mine_a, loc.at[0])
        keep_b = pltpu.make_async_copy(sb, mine_b, loc.at[1])
        keep_a.start()
        keep_b.start()

        def between(i):
            for g, at in enumerate(when):
                @pl.when(i == at)
                def _(g=g):
                    act(g + 1)
        sweep.run(lambda c: None, between)
        for k in list(range(20, 24)) + list(range(28, 40)):
            rc(*flat[k]).wait_recv()
        for k in range(40):
            rc(*flat[k]).wait_send()
        keep_a.wait()
        keep_b.wait()
        sweep.drain()

    dma = pltpu.SemaphoreType.DMA
    anyspec = pl.BlockSpec(memory_space=pl.ANY)
    S = jax.ShapeDtypeStruct
    return pl.pallas_call(
        kernel,
        in_specs=[anyspec] * 5,
        out_specs=[anyspec] * 4,
        out_shape=[S((nz, ny, ns, D), f32), S((nz, ny, ns, D), f32), S((D, nb * nblk), f32), S((nb * nblk, D), f32)],
        scratch_shapes=sweep_scratch(T, D, nb, tc) + [
            pltpu.VMEM((ns, D), bf16), pltpu.VMEM((ns, D), bf16), pltpu.VMEM((ns, D), f32), pltpu.VMEM((ns, D), f32),
            dma((2, nc)), dma((2,)), dma((2,)), dma((40,)), dma((40,))],
        compiler_params=pltpu.CompilerParams(collective_id=1, has_side_effects=True, vmem_limit_bytes=62 << 20),
        cost_estimate=pl.CostEstimate(flops=8 * nb * nblk * T * D, bytes_accessed=4 * T * D + 12 * nb * nblk * D, transcendentals=0),
        name="spread",
    )


def final_call(T, D, FF, n_dev, ns, nb, tc, sub, done):
    nc = T // tc
    n_loc = FF - ns * n_dev
    nblk = n_loc // nb - done
    n_sp = ns * n_dev
    turns = nblk * nc
    rows = 128
    tasks = done * nb // rows + n_sp // rows
    per = -(-tasks // turns)

    def kernel(rg, dhg, w1, w2, ga, gb, lu, ld, up, down, R, DH, w1b, w2b, o1, o2, uda, udb, wsem, osem,
               cu, cd, ct, lsem, isem, tsem):
        def token_copy(c):
            r = pl.ds(pl.multiple_of(c * tc, tc), tc)
            return (pltpu.make_async_copy(rg.at[r], R.at[r], lsem.at[0, c]),
                    pltpu.make_async_copy(dhg.at[r], DH.at[r], lsem.at[1, c]))
        sweep = Sweep(T, D, nb, tc, sub, nblk, done * nb, (R, DH, w1b, w2b, o1, o2, uda, udb, wsem, osem), w1, w2, up, down,
                      done * nb, done * nb)
        sweep.prefetch()
        for c in range(nc):
            for x in token_copy(c):
                x.start()
        n_l = done * nb // rows

        def ins(t, k):
            lo = pl.multiple_of(lax.min(t, n_l - 1) * rows, rows)
            sp = pl.multiple_of(lax.max(t - n_l, 0) * rows, rows)
            return ([pltpu.make_async_copy(ld.at[pl.ds(lo, rows), :], cd.at[k], isem.at[0, k]),
                     pltpu.make_async_copy(lu.at[:, pl.ds(lo, rows)], cu.at[k], isem.at[1, k])],
                    [pltpu.make_async_copy(gb.at[pl.ds(sp, rows), :], cd.at[k], isem.at[0, k]),
                     pltpu.make_async_copy(ga.at[pl.ds(sp, rows), :], ct.at[k], isem.at[1, k])])

        def outs(t, k):
            at = pl.multiple_of(jnp.where(t < n_l, t * rows, n_loc + (t - n_l) * rows), rows)
            return [pltpu.make_async_copy(cd.at[k], down.at[pl.ds(at, rows), :], tsem.at[0, k]),
                    pltpu.make_async_copy(cu.at[k], up.at[:, pl.ds(at, rows)], tsem.at[1, k])]

        def each(t, which):
            @pl.when(t < n_l)
            def _():
                for x in ins(t, lax.rem(t, 2 * per))[0]:
                    getattr(x, which)()

            @pl.when((t >= n_l) & (t < tasks))
            def _():
                for x in ins(t, lax.rem(t, 2 * per))[1]:
                    getattr(x, which)()

        def fetch(g):
            def one(k, _):
                each(g * per + k, "start")
                return 0
            lax.fori_loop(0, per, one, 0)

        def put(g):
            def one(k, _):
                t = g * per + k
                each(t, "wait")
                slot = lax.rem(t, 2 * per)

                @pl.when((t >= n_l) & (t < tasks))
                def _():
                    cu[slot] = ct[slot].T

                @pl.when(t < tasks)
                def _():
                    for x in outs(t, slot):
                        x.start()
                return 0
            lax.fori_loop(0, per, one, 0)

        def settle(g):
            def one(k, _):
                t = g * per + k

                @pl.when((t >= 0) & (t < tasks))
                def _():
                    for x in outs(t, lax.rem(t, 2 * per)):
                        x.wait()
                return 0
            lax.fori_loop(0, per, one, 0)
        fetch(0)

        def between(i):
            settle(i - 2)
            fetch(i)
            put(i - 1)
        sweep.run(lambda c: [x.wait() for x in token_copy(c)], between)
        settle(turns - 1)
        sweep.drain()

    dma = pltpu.SemaphoreType.DMA
    anyspec = pl.BlockSpec(memory_space=pl.ANY)
    S = jax.ShapeDtypeStruct
    return pl.pallas_call(
        kernel,
        in_specs=[anyspec] * 8,
        out_specs=[anyspec] * 2,
        out_shape=[S((D, FF), f32), S((FF, D), f32)],
        scratch_shapes=sweep_scratch(T, D, nb, tc) + [
            pltpu.VMEM((2 * per, D, rows), f32), pltpu.VMEM((2 * per, rows, D), f32), pltpu.VMEM((2 * per, rows, D), f32),
            dma((2, nc)), dma((2, 2 * per)), dma((2, 2 * per))],
        compiler_params=pltpu.CompilerParams(vmem_limit_bytes=63 << 20),
        cost_estimate=pl.CostEstimate(flops=8 * nb * nblk * T * D, bytes_accessed=4 * T * D + 24 * FF * D, transcendentals=0),
        name="final",
    )


def solution(mesh):
    n_stage = mesh.shape["stage"]
    n_data = mesh.shape["data"]
    ny = int(round(n_data ** 0.5))
    nz = n_data // ny
    ns, nb, tc, sub, done = 160, 256, 1024, 256, 11
    when = (8, 14, 18, 28, 38)

    def local_step(x_in, y_tgt, w_up, w_down, gain):
        n_micro, T, D = x_in.shape
        FF = w_up.shape[2]
        w1, w2 = w_up[0], w_down[0]
        tok_total = n_data * n_micro * T
        rg, dhg, wt1, _, dg, loss = chain_call(T, D, FF, ny, nz, n_stage, tok_total, 256, 4)(x_in, y_tgt, gain, w1, w2)
        rg = rg.reshape(tok_total, D)
        dhg = dhg.reshape(tok_total, D)
        ga, gb, lu, ld = spread_call(tok_total, D, FF, ny, nz, ns, nb, tc, sub, done, when)(rg, dhg, w1, w2, wt1)
        ga = ga.reshape(ns * n_data, D)
        gb = gb.reshape(ns * n_data, D)
        up, down = final_call(tok_total, D, FF, n_data, ns, nb, tc, sub, done)(rg, dhg, w1, w2, ga, gb, lu, ld)
        return up[None], down[None], dg, loss[0, :1]

    return jax.shard_map(local_step, mesh=mesh, in_specs=(P(("part", "data"), None, None), P(("part", "data"), None, None), P("stage", None, None), P("stage", None, None), P("stage", None)), out_specs=(P(("part", "stage"), None, None), P(("part", "stage"), None, None), P(("part", "stage"), None), P("part")), check_vma=False)
```

```python
import functools
import math

import jax
import jax.numpy as jnp
from jax import lax
from jax.experimental import pallas as pl
from jax.experimental.pallas import tpu as pltpu
from jax.sharding import PartitionSpec as P

EPS = 1e-6
C0 = math.sqrt(2.0 / math.pi)
CUB = 0.044715
f32 = jnp.float32
bf16 = jnp.bfloat16
MESH = pl.DeviceIdType.MESH
ROWS = (((0,), (0,)), ((), ()))
LASTS = (((1,), (1,)), ((), ()))


def gelu_u(a):
    t = jnp.tanh(C0 * (a + CUB * (a * a * a)))
    return a * (0.5 * (1.0 + t))


def gelu_both(a):
    a2 = a * a
    t = jnp.tanh(C0 * (a + CUB * (a2 * a)))
    half = 0.5 * (1.0 + t)
    slope = half + (0.5 * a) * (1.0 - t * t) * (C0 + (3.0 * CUB * C0) * a2)
    return a * half, slope


def inv_rms(x):
    return lax.rsqrt(jnp.mean(x * x, axis=-1, keepdims=True) + EPS)


NEEDS = ((), (0, 1, 2, 3), (4, 5, 6, 7), (8, 9, 10, 11), (12, 13, 14, 15, 16, 17, 18, 19), (24, 25, 26, 27))
LAST_ONES = tuple(range(20, 24)) + tuple(range(28, 40))


def ring_plan(z, y, nz, ny, mine, at):
    def plane(zz, yy):
        return {"data": lax.rem(zz + nz, nz) * ny + lax.rem(yy + ny, ny)}

    up = (plane(z, y + 1), plane(z + 1, y))
    dn = (plane(z, y - 1), plane(z - 1, y))
    plus = (lambda k: (z, lax.rem(y + k + ny, ny)), lambda k: (lax.rem(z + k + nz, nz), y))

    def cross(p, j, k):
        zz, yy = lax.rem(z + nz + (k if p == 0 else j), nz), lax.rem(y + ny + (j if p == 0 else k), ny)
        return (p, zz, yy)

    groups = []
    groups.append([(2 * p + d, mine(p), at(p, z, y, None), (up, dn)[d][p]) for p in (0, 1) for d in (0, 1)]
                  + [(4 + 2 * p + d, mine(p), at(p, z, y, None), (up, dn)[d][1 - p]) for p in (0, 1) for d in (0, 1)])

    def thru(k, where, half, dev):
        ref = at(*where, half)
        return (k, ref, ref, dev)
    g = [thru(8 + 2 * p + d, cross(p, (-1, 1)[d], 0), d, (up, dn)[d][p]) for p in (0, 1) for d in (0, 1)]
    g += [thru(12 + 4 * p + 2 * j + d, cross(p, (-1, 1)[j], 0), None, (up, dn)[d][1 - p]) for p in (0, 1) for j in (0, 1) for d in (0, 1)]
    groups.append(g)
    groups.append([thru(20 + 2 * p + d, cross(p, 0, (-1, 1)[d]), d, (up, dn)[d][1 - p]) for p in (0, 1) for d in (0, 1)])
    groups.append([thru(24 + 2 * p + d, cross(p, 2, 0), None, (up, dn)[d][1 - p]) for p in (0, 1) for d in (0, 1)])
    groups.append([thru(28 + 4 * p + 2 * j + d, cross(p, (-1, 1)[j], (-1, 1)[d]), d, (up, dn)[d][1 - p])
                   for p in (0, 1) for j in (0, 1) for d in (0, 1)])
    groups.append([thru(36 + 2 * p + d, cross(p, 2, (-1, 1)[d]), d, (up, dn)[d][1 - p]) for p in (0, 1) for d in (0, 1)])
    return groups


def chain_call(T, D, FF, ny, nz, n_stage, tok_total, cb, nj, nb, tc, n_pre, times, ahead):
    cw = FF // nj
    last = n_stage - 1
    h = T // 2
    qr = T // 4
    early = (n_stage * 3) // 8

    nc = tok_total // tc
    n_turn = n_pre // 2 * nc

    def kernel(x_ref, y_ref, g_ref, w1, w2, rg, dhg, wt1, wt2, ap, dg_o, loss_o,
               pbuf, qbuf, a_s, acc, xb, ob, rb, db, dxb, ts1, ts2, ast, lossb, exy, exz, dgacc,
               wsem, tsem1, tsem2, xs, xr, ds, dr_, ls, lr, ags, agr, own, exs, exr, rsem, asem):
        data = lax.axis_index("data")
        s = lax.axis_index("stage")
        z = data // ny
        y = lax.rem(data, ny)

        def plane(zz, yy):
            return {"data": lax.rem(zz + nz, nz) * ny + lax.rem(yy + ny, ny)}

        yp, ym = lax.rem(y + 1, ny), lax.rem(y + ny - 1, ny)
        zp, zm = lax.rem(z + 1, nz), lax.rem(z + nz - 1, nz)
        nxt = {"stage": lax.rem(s + 1, n_stage)}
        prv = {"stage": lax.rem(s + n_stage - 1, n_stage)}

        cp = pltpu.make_async_copy(w1, pbuf, wsem.at[0])
        cq = pltpu.make_async_copy(w2, qbuf, wsem.at[1])
        cp.start()
        cq.start()

        bar = pltpu.get_barrier_semaphore()
        for dev in [plane(z, y + k) for k in range(1, ny)] + [plane(z + k, y) for k in range(1, nz)] + [nxt, prv]:
            pl.semaphore_signal(bar, inc=1, device_id=dev, device_id_type=MESH)
        pl.semaphore_wait(bar, ny + nz)

        def rc(src, dst, ssem, rsem, dev):
            return pltpu.make_async_remote_copy(src_ref=src, dst_ref=dst, send_sem=ssem, recv_sem=rsem, device_id=dev, device_id_type=MESH)

        def ag(t, m, src, dst):
            def at(p, zz, yy, half):
                rows = pl.ds(p * h, h) if half is None else pl.ds(p * h + half * qr, qr)
                return dst.at[zz, yy, m, rows]
            groups = ring_plan(z, y, nz, ny, lambda p: src.at[m, pl.ds(p * h, h)], at)
            entry = {e[0]: e for group in groups for e in group}

            def copy(k):
                _, a, b, dev = entry[k]
                return rc(a, b, ags.at[t, m, k], agr.at[t, m, k], dev)

            def start(g):
                for k in NEEDS[g]:
                    copy(k).wait_recv()
                for e in groups[g]:
                    copy(e[0]).start()
                if g == 0:
                    pltpu.make_async_copy(src.at[m], dst.at[z, y, m], own.at[t, m]).start()

            def finish():
                for k in LAST_ONES:
                    copy(k).wait_recv()
                for k in range(40):
                    copy(k).wait_send()
                pltpu.make_async_copy(src.at[m], dst.at[z, y, m], own.at[t, m]).wait()
            return start, finish

        def ag_start(t, m, src, dst):
            ag(t, m, src, dst)[0](0)

        def ag_half(t, src, dst):
            for g in (1, 2, 3):
                for m in range(2):
                    ag(t, m, src, dst)[0](g)

        def ag_tail(t, src, dst):
            for g in (4, 5):
                for m in range(2):
                    ag(t, m, src, dst)[0](g)
            for m in range(2):
                ag(t, m, src, dst)[1]()

        def transposes():
            nb = FF // cb

            def cp1(c, slot):
                return pltpu.make_async_copy(ts1.at[slot], wt1.at[pl.ds(c * cb, cb), :], tsem1.at[slot])

            def cp2(c, slot):
                return pltpu.make_async_copy(ts2.at[slot], wt2.at[:, pl.ds(c * cb, cb)], tsem2.at[slot])

            def body(c, _):
                slot = lax.rem(c, 2)

                @pl.when(c >= 2)
                def _():
                    cp1(c - 2, slot).wait()
                    cp2(c - 2, slot).wait()
                off = pl.multiple_of(c * cb, cb)
                ts1[slot] = pbuf[:, pl.ds(off, cb)].T
                ts2[slot] = qbuf[pl.ds(off, cb), :].T
                cp1(c, slot).start()
                cp2(c, slot).start()
                return 0
            lax.fori_loop(0, nb, body, 0)
            for c in (nb - 2, nb - 1):
                cp1(c, c % 2).wait()
                cp2(c, c % 2).wait()

        gain = g_ref[...]

        def two_dots(first):
            def second(j, u):
                p = jnp.dot(u, qbuf[j * cw:(j + 1) * cw, :], preferred_element_type=f32)
                if j == 0:
                    acc[...] = p
                else:
                    acc[...] += p
            u = first(0)
            for j in range(1, nj):
                un = first(j)
                second(j - 1, u)
                u = un
            second(nj - 1, u)

        @pl.when(s == 0)
        def _():
            xb[...] = x_ref[...]
        lossb[...] = jnp.zeros_like(lossb)
        cp.wait()
        cq.wait()

        @pl.when(s >= early)
        def _():
            transposes()

        def x_send(m):
            return rc(ob.at[m], xb.at[m], xs.at[m], xr.at[m], nxt)

        def fwd(m, _):
            @pl.when(s > 0)
            def _():
                x_send(m).wait_recv()
            x = xb[m].astype(f32)
            r = (x * inv_rms(x) * gain).astype(bf16)
            rb[m] = r
            ag_start(0, m, rb, rg)

            def first(j):
                a = jnp.dot(r, pbuf[:, j * cw:(j + 1) * cw], preferred_element_type=f32)
                a_s[m, :, j * cw:(j + 1) * cw] = a
                return gelu_u(a).astype(bf16)
            two_dots(first)
            ob[m] = (xb[m].astype(f32) + acc[...]).astype(bf16)

            @pl.when(s < last)
            def _():
                x_send(m).start()

            @pl.when(s == last)
            def _():
                e = ob[m].astype(f32) - y_ref[m].astype(f32)
                lossb[...] += jnp.sum(e * e)
                db[m] = (e * (1.0 / tok_total)).astype(bf16)
            return 0
        lax.fori_loop(0, 2, fwd, 0)

        @pl.when(s < early)
        def _():
            transposes()
        bp = pltpu.make_async_copy(wt2, pbuf, wsem.at[0])
        bq = pltpu.make_async_copy(wt1, qbuf, wsem.at[1])

        @pl.when(s >= n_stage // 2)
        def _():
            bp.start()
            bq.start()

        def r_copy(i):
            dev, m = i // 2, lax.rem(i, 2)
            return pltpu.make_async_copy(rg.at[dev // ny, lax.rem(dev, ny), m], qbuf.at[pl.ds(pl.multiple_of(i * T, T), T), :], rsem.at[i])

        def r_start(i, _):
            r_copy(i).start()
            return 0

        def r_wait(i, _):
            r_copy(i).wait()
            return 0

        def a_copies(i):
            slot, pair = lax.rem(i, 2), i // nc
            rows = pl.ds(pl.multiple_of(lax.rem(i, nc) * tc, tc), tc)
            return [pltpu.make_async_copy(ast.at[slot, k], ap.at[2 * pair + k, rows, :], asem.at[slot, k]) for k in range(2)]

        def turns(lo, hi, tick):
            def turn(i, _):
                tick(i)

                @pl.when(i >= lo + 2)
                def _():
                    for c in a_copies(i - 2):
                        c.wait()
                slot, pair = lax.rem(i, 2), i // nc
                base = pl.multiple_of(lax.rem(i, nc) * tc, tc)
                for k in range(2):
                    cols = pl.ds(pl.multiple_of((2 * pair + k) * nb, nb), nb)
                    ast[slot, k] = jnp.dot(qbuf[pl.ds(base, tc), :], pbuf[:, cols], preferred_element_type=f32)
                for c in a_copies(i):
                    c.start()
                return 0
            lax.fori_loop(lo, hi, turn, 0)

            @pl.when(hi >= lo + 2)
            def _():
                for c in a_copies(hi - 2) + a_copies(hi - 1):
                    c.wait()
        n_early = jnp.where(s == 0, ahead[0], jnp.where(s == 1, ahead[1], jnp.where(s == 2, ahead[2], jnp.where(s == 3, ahead[3], 0))))

        l_send = rc(lossb, lossb, ls, lr, prv)

        @pl.when(s == last)
        def _():
            l_send.start()

        @pl.when(s < last)
        def _():
            ag_half(0, rb, rg)

        @pl.when(s < n_stage // 2)
        def _():
            ag_tail(0, rb, rg)
            lax.fori_loop(0, 2 * ny * nz, r_start, 0)
            lax.fori_loop(0, 2 * ny * nz, r_wait, 0)
            turns(0, n_early, lambda i: None)
            bp.start()
            bq.start()
        bp.wait()
        bq.wait()

        def d_send(m):
            return rc(dxb.at[m], db.at[m], ds.at[m], dr_.at[m], prv)

        dgacc[...] = jnp.zeros_like(dgacc)

        @pl.when(s == 0)
        def _():
            for m in range(2):
                d_send(m).wait_recv()
                ag_start(1, m, db, dhg)
            for m in range(2):
                ag(1, m, db, dhg)[0](1)

        def bwd(m, _):
            @pl.when((s < last) & (s > 0))
            def _():
                d_send(m).wait_recv()

            @pl.when(s > 0)
            def _():
                ag_start(1, m, db, dhg)
            dh = db[m]

            def first(j):
                du = jnp.dot(dh, pbuf[:, j * cw:(j + 1) * cw], preferred_element_type=f32)
                _, slope = gelu_both(a_s[m, :, j * cw:(j + 1) * cw])
                return (du * slope).astype(bf16)
            two_dots(first)
            x = xb[m].astype(f32)
            q = inv_rms(x)
            n = x * q
            dr = acc[...]
            dn = dr * gain
            dx = q * (dn - n * jnp.mean(dn * n, axis=-1, keepdims=True))
            dxb[m] = (db[m].astype(f32) + dx).astype(bf16)

            @pl.when(s > 0)
            def _():
                d_send(m).start()
            dgacc[...] += jnp.sum(dr * n, axis=0, keepdims=True)
            return 0
        lax.fori_loop(0, 2, bwd, 0)

        @pl.when(s < last)
        def _():
            l_send.wait_recv()

            @pl.when(s > 0)
            def _():
                l_send.start()

        exy[y, :, :D] = jnp.broadcast_to(dgacc[...], (8, D))
        exy[y, :, D:] = lossb[...]

        def ex(axis, k):
            buf, i, dev = (exy, y, plane(z, y + k)) if axis == 0 else (exz, z, plane(z + k, y))
            return rc(buf.at[i], buf.at[i], exs.at[axis, k - 1], exr.at[axis, k - 1], dev)
        for k in range(1, ny):
            ex(0, k).start()
        cw1 = pltpu.make_async_copy(w1, pbuf, wsem.at[0])
        cw1.start()

        @pl.when(s == last)
        def _():
            ag_half(0, rb, rg)

        @pl.when(s >= n_stage // 2)
        def _():
            ag_tail(0, rb, rg)

        lax.fori_loop(0, 2 * ny * nz, r_start, 0)
        lax.fori_loop(0, 2 * ny * nz, r_wait, 0)
        cw1.wait()

        def ex_mid():
            for k in range(1, ny):
                ex(0, k).wait_recv()
            tot = exy[0]
            for k in range(1, ny):
                tot = tot + exy[k]
            exz[z] = tot
            for k in range(1, nz):
                ex(1, k).start()

        def ex_last():
            for k in range(1, nz):
                ex(1, k).wait_recv()
            tot = exz[0]
            for k in range(1, nz):
                tot = tot + exz[k]
            dg_o[...] = tot[0:1, :D]
            loss_o[...] = tot[0:1, D:] * (1.0 / (tok_total * D))

        def later(g, m):
            return lambda: ag(1, m, db, dhg)[0](g)
        events = [later(1, 0), later(1, 1), ex_mid, later(2, 0), later(2, 1), later(3, 0), later(3, 1), later(4, 0), later(4, 1),
                  ex_last, later(5, 0), later(5, 1)]
        due = [n_early + jnp.where(s == 0, t0, jnp.where(s == 1, t1, jnp.where(s < n_stage // 2, t2, t3))) for t0, t1, t2, t3 in zip(*times)]

        def tick(i):
            for t, event in zip(due, events):
                @pl.when(i == t)
                def _(event=event):
                    event()
        turns(n_early, n_turn, tick)
        for m in range(2):
            ag(1, m, db, dhg)[1]()
        for axis, n in ((0, ny), (1, nz)):
            for k in range(1, n):
                ex(axis, k).wait_send()

        @pl.when(s < last)
        def _():
            x_send(0).wait_send()
            x_send(1).wait_send()

        @pl.when(s > 0)
        def _():
            d_send(0).wait_send()
            d_send(1).wait_send()
            l_send.wait_send()

    dma = pltpu.SemaphoreType.DMA
    anyspec = pl.BlockSpec(memory_space=pl.ANY)
    vspec = pl.BlockSpec(memory_space=pltpu.VMEM)
    S = jax.ShapeDtypeStruct
    return pl.pallas_call(
        kernel,
        in_specs=[vspec, vspec, vspec, anyspec, anyspec],
        out_specs=[anyspec, anyspec, anyspec, anyspec, anyspec, vspec, vspec],
        out_shape=[S((nz, ny, 2, T, D), bf16), S((nz, ny, 2, T, D), bf16), S((FF, D), bf16), S((D, FF), bf16),
                   S((n_pre, tok_total, nb), f32), S((1, D), f32), S((1, 128), f32)],
        scratch_shapes=[
            pltpu.VMEM((D, FF), bf16), pltpu.VMEM((FF, D), bf16), pltpu.VMEM((2, T, FF), f32), pltpu.VMEM((T, D), f32),
            pltpu.VMEM((2, T, D), bf16), pltpu.VMEM((2, T, D), bf16), pltpu.VMEM((2, T, D), bf16),
            pltpu.VMEM((2, T, D), bf16), pltpu.VMEM((2, T, D), bf16),
            pltpu.VMEM((2, cb, D), bf16), pltpu.VMEM((2, D, cb), bf16), pltpu.VMEM((2, 2, tc, nb), f32),
            pltpu.VMEM((8, 128), f32), pltpu.VMEM((ny, 8, D + 128), f32), pltpu.VMEM((nz, 8, D + 128), f32),
            pltpu.VMEM((1, D), f32),
            dma((2,)), dma((2,)), dma((2,)), dma((2,)), dma((2,)), dma((2,)), dma((2,)), dma, dma,
            dma((2, 2, 40)), dma((2, 2, 40)), dma((2, 2)), dma((2, 3)), dma((2, 3)), dma((2 * ny * nz,)), dma((2, 2))],
        compiler_params=pltpu.CompilerParams(collective_id=0, has_side_effects=True, vmem_limit_bytes=63 << 20),
        cost_estimate=pl.CostEstimate(flops=8 * 2 * T * D * FF * 2, bytes_accessed=6 * D * FF * 2, transcendentals=0),
        name="chain",
    )


class Sweep:
    def __init__(self, T, D, nb, tc, sub, nblk, off, refs, ap, wt2, out_up, out_down, up_off, down_off):
        self.T, self.D, self.nb, self.tc, self.sub, self.nblk = T, D, nb, tc, sub, nblk
        self.off, self.up_off, self.down_off = off, up_off, down_off
        self.nc = T // tc
        self.ap, self.wt2, self.out_up, self.out_down = ap, wt2, out_up, out_down
        self.R, self.DH, self.w2b, self.o1, self.o2, self.uda, self.udb, self.aba, self.abb, self.wsem, self.osem, self.asem = refs

    def wcopy(self, b):
        sl = lax.rem(b, 2)
        at = pl.multiple_of(self.off + b * self.nb, self.nb)
        return (pltpu.make_async_copy(self.wt2.at[:, pl.ds(at, self.nb)], self.w2b.at[sl], self.wsem.at[sl]),)

    def acopy(self, i, buf, slot):
        rows = pl.ds(pl.multiple_of(lax.rem(i, self.nc) * self.tc, self.tc), self.tc)
        return pltpu.make_async_copy(self.ap.at[self.off // self.nb + i // self.nc, rows, :], buf, self.asem.at[slot])

    def ocopy(self, b):
        sl = lax.rem(b, 2)
        up = pl.multiple_of(self.up_off + b * self.nb, self.nb)
        dn = pl.multiple_of(self.down_off + b * self.nb, self.nb)
        return (pltpu.make_async_copy(self.o1.at[sl], self.out_up.at[:, pl.ds(up, self.nb)], self.osem.at[0, sl]),
                pltpu.make_async_copy(self.o2.at[sl], self.out_down.at[pl.ds(dn, self.nb), :], self.osem.at[1, sl]))

    def ocopy(self, b):
        sl = lax.rem(b, 2)
        up = pl.multiple_of(self.up_off + b * self.nb, self.nb)
        dn = pl.multiple_of(self.down_off + b * self.nb, self.nb)
        return (pltpu.make_async_copy(self.o1.at[sl], self.out_up.at[:, pl.ds(up, self.nb)], self.osem.at[0, sl]),
                pltpu.make_async_copy(self.o2.at[sl], self.out_down.at[pl.ds(dn, self.nb), :], self.osem.at[1, sl]))

    def prefetch(self):
        for x in self.wcopy(0):
            x.start()
        self.acopy(0, self.aba, 0).start()

    def step(self, i, dst, src, pre):
        nb, tc, sub, D = self.nb, self.tc, self.sub, self.D
        c, sl = lax.rem(i, self.nc), lax.rem(i // self.nc, 2)
        j = i - 1
        jc, jl = lax.rem(j, self.nc), lax.rem(j // self.nc, 2)

        def first(k):
            base = pl.multiple_of(c * tc + k * sub, sub)
            a = pre[k * sub:(k + 1) * sub, :]
            du = jnp.dot(self.DH[pl.ds(base, sub), :], self.w2b[sl], preferred_element_type=f32)
            u, slope = gelu_both(a)
            dst[k * sub:(k + 1) * sub, :nb] = u.astype(bf16)
            dst[k * sub:(k + 1) * sub, nb:] = (du * slope).astype(bf16)

        def second(q):
            keep = jc > 0
            base = pl.multiple_of(jc * tc, tc)
            n = slice(q * 256, (q + 1) * 256)
            p2 = lax.dot_general(src[:, :nb], self.DH[pl.ds(base, tc), n], ROWS, preferred_element_type=f32)
            self.o2[jl, :, n] = jnp.where(keep, self.o2[jl, :, n], 0.0) + p2
            p1 = lax.dot_general(self.R[pl.ds(base, tc), n], src[:, nb:], ROWS, preferred_element_type=f32)
            self.o1[jl, n, :] = jnp.where(keep, self.o1[jl, n, :], 0.0) + p1
        q = 0
        for k in range(tc // sub):
            first(k)
            while src is not None and q < ((k + 1) * (D // 256)) // (tc // sub):
                second(q)
                q += 1

    def prime(self):
        for x in self.wcopy(0):
            x.start()
        self.acopy(0, self.aba, 0).start()
        self.acopy(1, self.abb, 1).start()

    def run(self, loads, between):
        n, nc = self.nblk * self.nc, self.nc
        if loads is not None:
            loads(0)
        for x in self.wcopy(0):
            x.wait()
        for x in self.wcopy(1):
            x.start()
        self.acopy(0, self.aba, 0).wait()
        self.step(0, self.uda, None, self.aba)

        def body(ii, _):
            i = 2 * ii + 1
            b, odd = i // nc, lax.rem(ii, nc // 2)
            between(ii)
            if loads is not None:
                @pl.when(ii < nc // 2)
                def _():
                    loads(i)

                    @pl.when(i + 1 < nc)
                    def _():
                        loads(i + 1)

            @pl.when(odd == 0)
            def _():
                @pl.when(b >= 1)
                def _():
                    for x in self.ocopy(b - 1):
                        x.start()

                @pl.when(b >= 2)
                def _():
                    for x in self.ocopy(b - 2):
                        x.wait()
            self.acopy(lax.min(i + 1, n - 1), self.aba, 0).start()
            self.acopy(i, self.abb, 1).wait()
            self.step(i, self.udb, self.uda, self.abb)

            @pl.when((odd == nc // 2 - 1) & (b + 1 < self.nblk))
            def _():
                for x in self.wcopy(b + 1):
                    x.wait()

                @pl.when(b + 2 < self.nblk)
                def _():
                    for x in self.wcopy(b + 2):
                        x.start()
            self.acopy(lax.min(i + 2, n - 1), self.abb, 1).start()
            self.acopy(lax.min(i + 1, n - 1), self.aba, 0).wait()
            self.step(i + 1, self.uda, self.udb, self.aba)
            return 0
        lax.fori_loop(0, n // 2, body, 0)
        self.acopy(n - 1, self.abb, 1).wait()
        for x in self.ocopy(self.nblk - 1):
            x.start()

    def drain(self):
        for b in (self.nblk - 2, self.nblk - 1):
            for x in self.ocopy(b):
                x.wait()


def sweep_scratch(T, D, nb, tc):
    dma = pltpu.SemaphoreType.DMA
    return [pltpu.VMEM((T, D), bf16), pltpu.VMEM((T, D), bf16), pltpu.VMEM((2, D, nb), bf16),
            pltpu.VMEM((2, D, nb), f32), pltpu.VMEM((2, nb, D), f32), pltpu.VMEM((tc, 2 * nb), bf16), pltpu.VMEM((tc, 2 * nb), bf16),
            pltpu.VMEM((tc, nb), f32), pltpu.VMEM((tc, nb), f32), dma((2,)), dma((2, 2)), dma((2,))]


def spread_call(T, D, FF, ny, nz, ns, nb, tc, sub, nblk, when):
    nc = T // tc
    n_loc = FF - ns * ny * nz

    def kernel(rg, dhg, ap, w1, wt2, ga, gb, lu, ld, R, DH, w2b, o1, o2, uda, udb, aba, abb, wsem, osem, asem,
               s1b, s2b, sb, sn, us, das, lsem, ssem, loc, snd, rcv):
        data = lax.axis_index("data")
        z = data // ny
        y = lax.rem(data, ny)

        def plane(zz, yy):
            return {"data": lax.rem(zz + nz, nz) * ny + lax.rem(yy + ny, ny)}

        yup, ydn, zup, zdn = plane(z, y + 1), plane(z, y - 1), plane(z + 1, y), plane(z - 1, y)
        start = pl.multiple_of(n_loc + data * ns, ns)
        sw = [pltpu.make_async_copy(w1.at[:, pl.ds(start, ns)], s1b, ssem.at[0]),
              pltpu.make_async_copy(wt2.at[:, pl.ds(start, ns)], s2b, ssem.at[1])]
        for x in sw:
            x.start()

        def token_copy(c):
            rows = pl.ds(pl.multiple_of(c * tc, tc), tc)
            return (pltpu.make_async_copy(rg.at[rows], R.at[rows], lsem.at[0, c]),
                    pltpu.make_async_copy(dhg.at[rows], DH.at[rows], lsem.at[1, c]))
        for c in range(nc):
            for x in token_copy(c):
                x.start()
        bar = pltpu.get_barrier_semaphore()
        for dev in (yup, ydn, zup, zdn):
            pl.semaphore_signal(bar, inc=1, device_id=dev, device_id_type=MESH)
        pl.semaphore_wait(bar, 4)
        sweep = Sweep(T, D, nb, tc, sub, nblk, 0, (R, DH, w2b, o1, o2, uda, udb, aba, abb, wsem, osem, asem), ap, wt2, lu, ld, 0, 0)
        sweep.prime()
        for x in sw:
            x.wait()

        def own(c, _):
            for x in token_copy(c):
                x.wait()
            base = pl.multiple_of(c * tc, tc)
            for k in range(tc // sub):
                at = pl.ds(pl.multiple_of(base + k * sub, sub), sub)
                a = jnp.dot(R[at, :], s1b[...], preferred_element_type=f32)
                du = jnp.dot(DH[at, :], s2b[...], preferred_element_type=f32)
                u, slope = gelu_both(a)
                us[at, :] = u.astype(bf16)
                das[at, :] = (du * slope).astype(bf16)
            return 0

        def at(p, zz, yy, half):
            buf, n = ((ga, D), (gb, ns))[p]
            return buf.at[zz, yy] if half is None else buf.at[zz, yy, pl.ds(half * (n // 2), n // 2), :]
        plan = ring_plan(z, y, nz, ny, lambda p: (sn, sb)[p], at)
        entry = {e[0]: e for group in plan for e in group}

        def copy(k):
            _, a, b, dev = entry[k]
            return pltpu.make_async_remote_copy(src_ref=a, dst_ref=b, send_sem=snd.at[k], recv_sem=rcv.at[k], device_id=dev, device_id_type=MESH)

        def act(g):
            for k in NEEDS[g]:
                copy(k).wait_recv()
            for e in plan[g]:
                copy(e[0]).start()
        keep_a = pltpu.make_async_copy(sn, ga.at[z, y], loc.at[0])
        keep_b = pltpu.make_async_copy(sb, gb.at[z, y], loc.at[1])
        lax.fori_loop(0, nc, own, 0)
        sb[...] = lax.dot_general(us[...], DH[...], ROWS, preferred_element_type=f32)
        for k in (2, 3):
            copy(k).start()
        keep_b.start()
        sn[...] = lax.dot_general(das[...], R[...], ROWS, preferred_element_type=f32).T
        for k in (0, 1, 4, 5, 6, 7):
            copy(k).start()
        keep_a.start()

        def between(ii):
            hit = ii == when[0]
            for t in when[1:]:
                hit = hit | (ii == t)

            @pl.when(hit)
            def _():
                for g, t in enumerate(when):
                    @pl.when(ii == t)
                    def _(g=g):
                        act(g + 1)
        sweep.run(None, between)
        for k in LAST_ONES:
            copy(k).wait_recv()
        for k in range(40):
            copy(k).wait_send()
        keep_a.wait()
        keep_b.wait()
        sweep.drain()

    dma = pltpu.SemaphoreType.DMA
    anyspec = pl.BlockSpec(memory_space=pl.ANY)
    S = jax.ShapeDtypeStruct
    return pl.pallas_call(
        kernel,
        in_specs=[anyspec] * 5,
        out_specs=[anyspec] * 4,
        out_shape=[S((nz, ny, D, ns), f32), S((nz, ny, ns, D), f32), S((D, nb * nblk), f32), S((nb * nblk, D), f32)],
        scratch_shapes=sweep_scratch(T, D, nb, tc) + [
            pltpu.VMEM((D, ns), bf16), pltpu.VMEM((D, ns), bf16), pltpu.VMEM((ns, D), f32), pltpu.VMEM((D, ns), f32),
            pltpu.VMEM((T, ns), bf16), pltpu.VMEM((T, ns), bf16), dma((2, nc)), dma((2,)), dma((2,)), dma((40,)), dma((40,))],
        compiler_params=pltpu.CompilerParams(collective_id=1, has_side_effects=True, vmem_limit_bytes=62 << 20),
        cost_estimate=pl.CostEstimate(flops=8 * nb * nblk * T * D, bytes_accessed=4 * T * D + 12 * nb * nblk * D, transcendentals=0),
        name="spread",
    )


def final_call(T, D, FF, n_dev, ns, nb, tc, sub, done):
    nc = T // tc
    n_loc = FF - ns * n_dev
    nblk = n_loc // nb - done
    n_sp = ns * n_dev
    pairs = nblk * nc // 2
    rows = ns
    tasks = done * nb // rows + n_dev
    per = -(-tasks // pairs)

    def kernel(rg, dhg, ap, wt2, ga, gb, lu, ld, up, down, R, DH, w2b, o1, o2, uda, udb, aba, abb, wsem, osem, asem,
               cu, cd, lsem, isem, tsem):
        def token_copy(c):
            r = pl.ds(pl.multiple_of(c * tc, tc), tc)
            return (pltpu.make_async_copy(rg.at[r], R.at[r], lsem.at[0, c]),
                    pltpu.make_async_copy(dhg.at[r], DH.at[r], lsem.at[1, c]))
        sweep = Sweep(T, D, nb, tc, sub, nblk, done * nb, (R, DH, w2b, o1, o2, uda, udb, aba, abb, wsem, osem, asem), ap, wt2, up, down,
                      done * nb, done * nb)
        sweep.prime()
        for c in range(nc):
            for x in token_copy(c):
                x.start()
        n_l = done * nb // rows

        def ins(t, k):
            lo = pl.multiple_of(lax.min(t, n_l - 1) * rows, rows)
            sp = lax.max(t - n_l, 0)
            return ([pltpu.make_async_copy(ld.at[pl.ds(lo, rows), :], cd.at[k], isem.at[0, k]),
                     pltpu.make_async_copy(lu.at[:, pl.ds(lo, rows)], cu.at[k], isem.at[1, k])],
                    [pltpu.make_async_copy(gb.at[sp], cd.at[k], isem.at[0, k]),
                     pltpu.make_async_copy(ga.at[sp], cu.at[k], isem.at[1, k])])

        def outs(t, k):
            at = pl.multiple_of(jnp.where(t < n_l, t * rows, n_loc + (t - n_l) * rows), rows)
            return [pltpu.make_async_copy(cd.at[k], down.at[pl.ds(at, rows), :], tsem.at[0, k]),
                    pltpu.make_async_copy(cu.at[k], up.at[:, pl.ds(at, rows)], tsem.at[1, k])]

        def loop(g, what):
            def one(k, _):
                t = g * per + k

                @pl.when((t >= 0) & (t < tasks))
                def _():
                    what(t, lax.rem(t + 2 * per, 2 * per))
                return 0
            lax.fori_loop(0, per, one, 0)

        def fetch(t, k):
            @pl.when(t < n_l)
            def _():
                for x in ins(t, k)[0]:
                    x.start(priority=1)

            @pl.when(t >= n_l)
            def _():
                for x in ins(t, k)[1]:
                    x.start(priority=1)

        def put(t, k):
            for x in ins(t, k)[0]:
                x.wait()
            for x in outs(t, k):
                x.start(priority=1)

        def settle(t, k):
            for x in outs(t, k):
                x.wait()

        def between(ii):
            loop(ii - 1, settle)
            loop(ii + 1, fetch)
            loop(ii, put)
        loop(0, fetch)
        sweep.run(lambda c: [x.wait() for x in token_copy(c)], between)
        loop(pairs - 1, settle)
        sweep.drain()

    dma = pltpu.SemaphoreType.DMA
    anyspec = pl.BlockSpec(memory_space=pl.ANY)
    S = jax.ShapeDtypeStruct
    return pl.pallas_call(
        kernel,
        in_specs=[anyspec] * 8,
        out_specs=[anyspec] * 2,
        out_shape=[S((D, FF), f32), S((FF, D), f32)],
        scratch_shapes=sweep_scratch(T, D, nb, tc) + [
            pltpu.VMEM((2 * per, D, rows), f32), pltpu.VMEM((2 * per, rows, D), f32),
            dma((2, nc)), dma((2, 2 * per)), dma((2, 2 * per))],
        compiler_params=pltpu.CompilerParams(vmem_limit_bytes=63 << 20),
        cost_estimate=pl.CostEstimate(flops=8 * nb * nblk * T * D, bytes_accessed=4 * T * D + 24 * FF * D, transcendentals=0),
        name="final",
    )


def solution(mesh):
    n_stage = mesh.shape["stage"]
    n_data = mesh.shape["data"]
    ny = int(round(n_data ** 0.5))
    nz = n_data // ny
    ns, nb, tc, sub, done = 128, 256, 1024, 256, 12
    when = (4, 7, 9, 15, 20)
    times = ((-99, -99, 1, 0, 0, 0, 1, 3, 6, 6, 9, 11), (0, 2, 2, 4, 4, 6, 8, 11, 14, 14, 17, 20), (0, 1, 1, 3, 3, 5, 7, 10, 12, 12, 15, 17), (0, 0, 1, 2, 3, 5, 7, 11, 14, 14, 17, 20))
    ahead = (18, 10, 12, 8)

    def local_step(x_in, y_tgt, w_up, w_down, gain):
        n_micro, T, D = x_in.shape
        FF = w_up.shape[2]
        w1, w2 = w_up[0], w_down[0]
        tok_total = n_data * n_micro * T
        n_pre = (FF - ns * n_data) // nb
        rg, dhg, _, wt2, ap, dg, loss = chain_call(T, D, FF, ny, nz, n_stage, tok_total, 256, 4, nb, tc, n_pre, times, ahead)(x_in, y_tgt, gain, w1, w2)
        rg = rg.reshape(tok_total, D)
        dhg = dhg.reshape(tok_total, D)
        ga, gb, lu, ld = spread_call(tok_total, D, FF, ny, nz, ns, nb, tc, sub, done, when)(rg, dhg, ap, w1, wt2)
        ga = ga.reshape(n_data, D, ns)
        gb = gb.reshape(n_data, ns, D)
        up, down = final_call(tok_total, D, FF, n_data, ns, nb, tc, sub, done)(rg, dhg, ap, wt2, ga, gb, lu, ld)
        return up[None], down[None], dg, loss[0, :1]

    return jax.shard_map(local_step, mesh=mesh, in_specs=(P(("part", "data"), None, None), P(("part", "data"), None, None), P("stage", None, None), P("stage", None, None), P("stage", None)), out_specs=(P(("part", "stage"), None, None), P(("part", "stage"), None, None), P(("part", "stage"), None), P("part")), check_vma=False)
```

```python
import functools
import math

import jax
import jax.numpy as jnp
from jax import lax
from jax.experimental import pallas as pl
from jax.experimental.pallas import tpu as pltpu
from jax.sharding import PartitionSpec as P

EPS = 1e-6
C0 = math.sqrt(2.0 / math.pi)
CUB = 0.044715
f32 = jnp.float32
bf16 = jnp.bfloat16
MESH = pl.DeviceIdType.MESH
ROWS = (((0,), (0,)), ((), ()))
LASTS = (((1,), (1,)), ((), ()))


def gelu_u(a):
    t = jnp.tanh(C0 * (a + CUB * (a * a * a)))
    return a * (0.5 * (1.0 + t))


def gelu_both(a):
    a2 = a * a
    t = jnp.tanh(C0 * (a + CUB * (a2 * a)))
    half = 0.5 * (1.0 + t)
    slope = half + (0.5 * a) * (1.0 - t * t) * (C0 + (3.0 * CUB * C0) * a2)
    return a * half, slope


def inv_rms(x):
    return lax.rsqrt(jnp.mean(x * x, axis=-1, keepdims=True) + EPS)


NEEDS = ((), (0, 1, 2, 3), (4, 5, 6, 7), (8, 9, 10, 11), (12, 13, 14, 15, 16, 17, 18, 19), (24, 25, 26, 27))
LAST_ONES = tuple(range(20, 24)) + tuple(range(28, 40))


def ring_plan(z, y, nz, ny, mine, at):
    def plane(zz, yy):
        return {"data": lax.rem(zz + nz, nz) * ny + lax.rem(yy + ny, ny)}

    up = (plane(z, y + 1), plane(z + 1, y))
    dn = (plane(z, y - 1), plane(z - 1, y))
    plus = (lambda k: (z, lax.rem(y + k + ny, ny)), lambda k: (lax.rem(z + k + nz, nz), y))

    def cross(p, j, k):
        zz, yy = lax.rem(z + nz + (k if p == 0 else j), nz), lax.rem(y + ny + (j if p == 0 else k), ny)
        return (p, zz, yy)

    groups = []
    groups.append([(2 * p + d, mine(p), at(p, z, y, None), (up, dn)[d][p]) for p in (0, 1) for d in (0, 1)]
                  + [(4 + 2 * p + d, mine(p), at(p, z, y, None), (up, dn)[d][1 - p]) for p in (0, 1) for d in (0, 1)])

    def thru(k, where, half, dev):
        ref = at(*where, half)
        return (k, ref, ref, dev)
    g = [thru(8 + 2 * p + d, cross(p, (-1, 1)[d], 0), d, (up, dn)[d][p]) for p in (0, 1) for d in (0, 1)]
    g += [thru(12 + 4 * p + 2 * j + d, cross(p, (-1, 1)[j], 0), None, (up, dn)[d][1 - p]) for p in (0, 1) for j in (0, 1) for d in (0, 1)]
    groups.append(g)
    groups.append([thru(20 + 2 * p + d, cross(p, 0, (-1, 1)[d]), d, (up, dn)[d][1 - p]) for p in (0, 1) for d in (0, 1)])
    groups.append([thru(24 + 2 * p + d, cross(p, 2, 0), None, (up, dn)[d][1 - p]) for p in (0, 1) for d in (0, 1)])
    groups.append([thru(28 + 4 * p + 2 * j + d, cross(p, (-1, 1)[j], (-1, 1)[d]), d, (up, dn)[d][1 - p])
                   for p in (0, 1) for j in (0, 1) for d in (0, 1)])
    groups.append([thru(36 + 2 * p + d, cross(p, 2, (-1, 1)[d]), d, (up, dn)[d][1 - p]) for p in (0, 1) for d in (0, 1)])
    return groups


def chain_call(T, D, FF, ny, nz, n_stage, tok_total, cb, nj, nb, tc, n_pre, times, ahead):
    cw = FF // nj
    last = n_stage - 1
    h = T // 2
    qr = T // 4
    early = (n_stage * 3) // 8

    nc = tok_total // tc
    n_turn = n_pre // 2 * nc

    def kernel(x_ref, y_ref, g_ref, w1, w2, rg, dhg, wt1, wt2, ap, dg_o, loss_o,
               pbuf, qbuf, a_s, acc, xb, ob, rb, db, dxb, ts1, ts2, ast, lossb, exy, exz, dgacc,
               wsem, tsem1, tsem2, xs, xr, ds, dr_, ls, lr, ags, agr, own, exs, exr, rsem, asem):
        data = lax.axis_index("data")
        s = lax.axis_index("stage")
        z = data // ny
        y = lax.rem(data, ny)

        def plane(zz, yy):
            return {"data": lax.rem(zz + nz, nz) * ny + lax.rem(yy + ny, ny)}

        yp, ym = lax.rem(y + 1, ny), lax.rem(y + ny - 1, ny)
        zp, zm = lax.rem(z + 1, nz), lax.rem(z + nz - 1, nz)
        nxt = {"stage": lax.rem(s + 1, n_stage)}
        prv = {"stage": lax.rem(s + n_stage - 1, n_stage)}

        def part(j):
            return pl.ds(pl.multiple_of(j * cw, cw), cw)

        def weights(src_p, src_q, j):
            return (pltpu.make_async_copy(src_p.at[:, part(j)], pbuf.at[:, part(j)], wsem.at[0, j]),
                    pltpu.make_async_copy(src_q.at[part(j), :], qbuf.at[part(j), :], wsem.at[1, j]))

        def each_weight(src_p, src_q, what):
            def one(j, _):
                for x in weights(src_p, src_q, j):
                    getattr(x, what)()
                return 0
            lax.fori_loop(0, nj, one, 0)
        each_weight(w1, w2, "start")

        bar = pltpu.get_barrier_semaphore()
        for dev in [plane(z, y + k) for k in range(1, ny)] + [plane(z + k, y) for k in range(1, nz)] + [nxt, prv]:
            pl.semaphore_signal(bar, inc=1, device_id=dev, device_id_type=MESH)
        pl.semaphore_wait(bar, ny + nz)

        def rc(src, dst, ssem, rsem, dev):
            return pltpu.make_async_remote_copy(src_ref=src, dst_ref=dst, send_sem=ssem, recv_sem=rsem, device_id=dev, device_id_type=MESH)

        def ag(t, m, src, dst):
            def at(p, zz, yy, half):
                rows = pl.ds(p * h, h) if half is None else pl.ds(p * h + half * qr, qr)
                return dst.at[zz, yy, m, rows]
            groups = ring_plan(z, y, nz, ny, lambda p: src.at[m, pl.ds(p * h, h)], at)
            entry = {e[0]: e for group in groups for e in group}

            def copy(k):
                _, a, b, dev = entry[k]
                return rc(a, b, ags.at[t, m, k], agr.at[t, m, k], dev)

            def start(g):
                for k in NEEDS[g]:
                    copy(k).wait_recv()
                for e in groups[g]:
                    copy(e[0]).start()
                if g == 0:
                    pltpu.make_async_copy(src.at[m], dst.at[z, y, m], own.at[t, m]).start()

            def finish():
                for k in LAST_ONES:
                    copy(k).wait_recv()
                for k in range(40):
                    copy(k).wait_send()
                pltpu.make_async_copy(src.at[m], dst.at[z, y, m], own.at[t, m]).wait()
            return start, finish

        def ag_start(t, m, src, dst):
            ag(t, m, src, dst)[0](0)

        def ag_half(t, src, dst):
            for g in (1, 2, 3):
                for m in range(2):
                    ag(t, m, src, dst)[0](g)

        def ag_tail(t, src, dst):
            for g in (4, 5):
                for m in range(2):
                    ag(t, m, src, dst)[0](g)
            for m in range(2):
                ag(t, m, src, dst)[1]()

        def transposes():
            nb = FF // cb

            def cp1(c, slot):
                return pltpu.make_async_copy(ts1.at[slot], wt1.at[pl.ds(c * cb, cb), :], tsem1.at[slot])

            def cp2(c, slot):
                return pltpu.make_async_copy(ts2.at[slot], wt2.at[:, pl.ds(c * cb, cb)], tsem2.at[slot])

            def body(c, _):
                slot = lax.rem(c, 2)

                @pl.when(c >= 2)
                def _():
                    cp1(c - 2, slot).wait()
                    cp2(c - 2, slot).wait()
                off = pl.multiple_of(c * cb, cb)
                ts1[slot] = pbuf[:, pl.ds(off, cb)].T
                ts2[slot] = qbuf[pl.ds(off, cb), :].T
                cp1(c, slot).start()
                cp2(c, slot).start()
                return 0
            lax.fori_loop(0, nb, body, 0)
            for c in (nb - 2, nb - 1):
                cp1(c, c % 2).wait()
                cp2(c, c % 2).wait()

        gain = g_ref[...]

        def two_dots(first, slow, src_p, src_q):
            @pl.when(slow)
            def _():
                def one(j, _):
                    for x in weights(src_p, src_q, j):
                        x.wait()
                    p = jnp.dot(first(j), qbuf[part(j), :], preferred_element_type=f32)
                    acc[...] = jnp.where(j > 0, acc[...], 0.0) + p
                    return 0
                lax.fori_loop(0, nj, one, 0)

            @pl.when(jnp.logical_not(slow))
            def _():
                fast_dots(first)

        def fast_dots(first):
            def second(j, u):
                p = jnp.dot(u, qbuf[j * cw:(j + 1) * cw, :], preferred_element_type=f32)
                if j == 0:
                    acc[...] = p
                else:
                    acc[...] += p
            u = first(0)
            for j in range(1, nj):
                un = first(j)
                second(j - 1, u)
                u = un
            second(nj - 1, u)

        @pl.when(s == 0)
        def _():
            xb[...] = x_ref[...]
        lossb[...] = jnp.zeros_like(lossb)

        @pl.when(s > 0)
        def _():
            each_weight(w1, w2, "wait")

        @pl.when(s >= early)
        def _():
            transposes()

        def x_send(m):
            return rc(ob.at[m], xb.at[m], xs.at[m], xr.at[m], nxt)

        def fwd(m, _):
            @pl.when(s > 0)
            def _():
                x_send(m).wait_recv()
            x = xb[m].astype(f32)
            r = (x * inv_rms(x) * gain).astype(bf16)
            rb[m] = r
            ag_start(0, m, rb, rg)

            def first(j):
                a = jnp.dot(rb[m], pbuf[:, part(j)], preferred_element_type=f32)
                a_s[m, :, part(j)] = a
                return gelu_u(a).astype(bf16)
            two_dots(first, (s == 0) & (m == 0), w1, w2)
            ob[m] = (xb[m].astype(f32) + acc[...]).astype(bf16)

            @pl.when(s < last)
            def _():
                x_send(m).start()

            @pl.when(s == last)
            def _():
                e = ob[m].astype(f32) - y_ref[m].astype(f32)
                lossb[...] += jnp.sum(e * e)
                db[m] = (e * (1.0 / tok_total)).astype(bf16)
            return 0
        lax.fori_loop(0, 2, fwd, 0)

        @pl.when(s < early)
        def _():
            transposes()
        @pl.when(s >= n_stage // 2)
        def _():
            each_weight(wt2, wt1, "start")

        def r_copy(i):
            dev, m = i // 2, lax.rem(i, 2)
            return pltpu.make_async_copy(rg.at[dev // ny, lax.rem(dev, ny), m], qbuf.at[pl.ds(pl.multiple_of(i * T, T), T), :], rsem.at[i])

        def r_start(i, _):
            r_copy(i).start()
            return 0

        def r_wait(i, _):
            r_copy(i).wait()
            return 0

        def a_copies(i):
            slot, pair = lax.rem(i, 2), i // nc
            rows = pl.ds(pl.multiple_of(lax.rem(i, nc) * tc, tc), tc)
            return [pltpu.make_async_copy(ast.at[slot, k], ap.at[2 * pair + k, rows, :], asem.at[slot, k]) for k in range(2)]

        def turns(lo, hi, tick, whole):
            def turn(i, _):
                tick(i)

                @pl.when(i >= lo + 2)
                def _():
                    for c in a_copies(i - 2):
                        c.wait()
                slot, pair = lax.rem(i, 2), i // nc
                base = pl.multiple_of(lax.rem(i, nc) * tc, tc)

                def block(k, _):
                    cols = pl.ds(pl.multiple_of((2 * pair + k) * nb, nb), nb)
                    ast[slot, k] = jnp.dot(qbuf[pl.ds(base, tc), :], pbuf[:, cols], preferred_element_type=f32)
                    return 0
                if whole:
                    block(0, 0)
                    block(1, 0)
                else:
                    lax.fori_loop(0, 2, block, 0)
                for c in a_copies(i):
                    c.start()
                return 0
            lax.fori_loop(lo, hi, turn, 0)

            @pl.when(hi >= lo + 2)
            def _():
                for c in a_copies(hi - 2) + a_copies(hi - 1):
                    c.wait()
        n_early = jnp.where(s == 0, ahead[0], jnp.where(s == 1, ahead[1], jnp.where(s == 2, ahead[2], jnp.where(s == 3, ahead[3], 0))))

        l_send = rc(lossb, lossb, ls, lr, prv)

        @pl.when(s == last)
        def _():
            l_send.start()

        @pl.when(s < last)
        def _():
            ag_half(0, rb, rg)

        @pl.when(s < n_stage // 2)
        def _():
            ag_tail(0, rb, rg)
            lax.fori_loop(0, 2 * ny * nz, r_start, 0)
            lax.fori_loop(0, 2 * ny * nz, r_wait, 0)
            turns(0, n_early, lambda i: None, False)
            each_weight(wt2, wt1, "start")

        @pl.when(s < last)
        def _():
            each_weight(wt2, wt1, "wait")

        def d_send(m):
            return rc(dxb.at[m], db.at[m], ds.at[m], dr_.at[m], prv)

        dgacc[...] = jnp.zeros_like(dgacc)

        @pl.when(s == 0)
        def _():
            for m in range(2):
                d_send(m).wait_recv()
                ag_start(1, m, db, dhg)
            for m in range(2):
                ag(1, m, db, dhg)[0](1)

        def bwd(m, _):
            @pl.when((s < last) & (s > 0))
            def _():
                d_send(m).wait_recv()

            @pl.when(s > 0)
            def _():
                ag_start(1, m, db, dhg)

            def first(j):
                du = jnp.dot(db[m], pbuf[:, part(j)], preferred_element_type=f32)
                _, slope = gelu_both(a_s[m, :, part(j)])
                return (du * slope).astype(bf16)
            two_dots(first, (s == last) & (m == 0), wt2, wt1)
            x = xb[m].astype(f32)
            q = inv_rms(x)
            n = x * q
            dr = acc[...]
            dn = dr * gain
            dx = q * (dn - n * jnp.mean(dn * n, axis=-1, keepdims=True))
            dxb[m] = (db[m].astype(f32) + dx).astype(bf16)

            @pl.when(s > 0)
            def _():
                d_send(m).start()
            dgacc[...] += jnp.sum(dr * n, axis=0, keepdims=True)
            return 0
        lax.fori_loop(0, 2, bwd, 0)

        @pl.when(s < last)
        def _():
            l_send.wait_recv()

            @pl.when(s > 0)
            def _():
                l_send.start()

        exy[y, :, :D] = jnp.broadcast_to(dgacc[...], (8, D))
        exy[y, :, D:] = lossb[...]

        def ex(axis, k):
            buf, i, dev = (exy, y, plane(z, y + k)) if axis == 0 else (exz, z, plane(z + k, y))
            return rc(buf.at[i], buf.at[i], exs.at[axis, k - 1], exr.at[axis, k - 1], dev)
        for k in range(1, ny):
            ex(0, k).start()
        cw1 = pltpu.make_async_copy(w1, pbuf, wsem.at[0, 0])
        cw1.start()

        @pl.when(s == last)
        def _():
            ag_half(0, rb, rg)

        @pl.when(s >= n_stage // 2)
        def _():
            ag_tail(0, rb, rg)

        lax.fori_loop(0, 2 * ny * nz, r_start, 0)
        lax.fori_loop(0, 2 * ny * nz, r_wait, 0)
        cw1.wait()

        def ex_mid():
            for k in range(1, ny):
                ex(0, k).wait_recv()
            tot = exy[0]
            for k in range(1, ny):
                tot = tot + exy[k]
            exz[z] = tot
            for k in range(1, nz):
                ex(1, k).start()

        def ex_last():
            for k in range(1, nz):
                ex(1, k).wait_recv()
            tot = exz[0]
            for k in range(1, nz):
                tot = tot + exz[k]
            dg_o[...] = tot[0:1, :D]
            loss_o[...] = tot[0:1, D:] * (1.0 / (tok_total * D))

        def later(g, m):
            return lambda: ag(1, m, db, dhg)[0](g)
        events = [later(1, 0), later(1, 1), ex_mid, later(2, 0), later(2, 1), later(3, 0), later(3, 1), later(4, 0), later(4, 1),
                  ex_last, later(5, 0), later(5, 1)]
        due = [n_early + jnp.where(s == 0, t0, jnp.where(s == 1, t1, jnp.where(s < n_stage // 2, t2, t3))) for t0, t1, t2, t3 in zip(*times)]

        def tick(i):
            for t, event in zip(due, events):
                @pl.when(i == t)
                def _(event=event):
                    event()
        turns(n_early, n_turn, tick, True)
        for m in range(2):
            ag(1, m, db, dhg)[1]()
        for axis, n in ((0, ny), (1, nz)):
            for k in range(1, n):
                ex(axis, k).wait_send()

        @pl.when(s < last)
        def _():
            x_send(0).wait_send()
            x_send(1).wait_send()

        @pl.when(s > 0)
        def _():
            d_send(0).wait_send()
            d_send(1).wait_send()
            l_send.wait_send()

    dma = pltpu.SemaphoreType.DMA
    anyspec = pl.BlockSpec(memory_space=pl.ANY)
    vspec = pl.BlockSpec(memory_space=pltpu.VMEM)
    S = jax.ShapeDtypeStruct
    return pl.pallas_call(
        kernel,
        in_specs=[vspec, vspec, vspec, anyspec, anyspec],
        out_specs=[anyspec, anyspec, anyspec, anyspec, anyspec, vspec, vspec],
        out_shape=[S((nz, ny, 2, T, D), bf16), S((nz, ny, 2, T, D), bf16), S((FF, D), bf16), S((D, FF), bf16),
                   S((n_pre, tok_total, nb), f32), S((1, D), f32), S((1, 128), f32)],
        scratch_shapes=[
            pltpu.VMEM((D, FF), bf16), pltpu.VMEM((FF, D), bf16), pltpu.VMEM((2, T, FF), f32), pltpu.VMEM((T, D), f32),
            pltpu.VMEM((2, T, D), bf16), pltpu.VMEM((2, T, D), bf16), pltpu.VMEM((2, T, D), bf16),
            pltpu.VMEM((2, T, D), bf16), pltpu.VMEM((2, T, D), bf16),
            pltpu.VMEM((2, cb, D), bf16), pltpu.VMEM((2, D, cb), bf16), pltpu.VMEM((2, 2, tc, nb), f32),
            pltpu.VMEM((8, 128), f32), pltpu.VMEM((ny, 8, D + 128), f32), pltpu.VMEM((nz, 8, D + 128), f32),
            pltpu.VMEM((1, D), f32),
            dma((2, nj)), dma((2,)), dma((2,)), dma((2,)), dma((2,)), dma((2,)), dma((2,)), dma, dma,
            dma((2, 2, 40)), dma((2, 2, 40)), dma((2, 2)), dma((2, 3)), dma((2, 3)), dma((2 * ny * nz,)), dma((2, 2))],
        compiler_params=pltpu.CompilerParams(collective_id=0, has_side_effects=True, vmem_limit_bytes=63 << 20),
        cost_estimate=pl.CostEstimate(flops=8 * 2 * T * D * FF * 2, bytes_accessed=6 * D * FF * 2, transcendentals=0),
        name="chain",
    )


class Sweep:
    def __init__(self, T, D, nb, tc, sub, nblk, off, refs, ap, wt2, out_up, out_down, up_off, down_off):
        self.T, self.D, self.nb, self.tc, self.sub, self.nblk = T, D, nb, tc, sub, nblk
        self.off, self.up_off, self.down_off = off, up_off, down_off
        self.nc = T // tc
        self.ap, self.wt2, self.out_up, self.out_down = ap, wt2, out_up, out_down
        self.R, self.DH, self.w2b, self.o1, self.o2, self.uda, self.udb, self.aba, self.abb, self.wsem, self.osem, self.asem = refs

    def wcopy(self, b):
        sl = lax.rem(b, 2)
        at = pl.multiple_of(self.off + b * self.nb, self.nb)
        return (pltpu.make_async_copy(self.wt2.at[:, pl.ds(at, self.nb)], self.w2b.at[sl], self.wsem.at[sl]),)

    def acopy(self, i, buf, slot):
        rows = pl.ds(pl.multiple_of(lax.rem(i, self.nc) * self.tc, self.tc), self.tc)
        return pltpu.make_async_copy(self.ap.at[self.off // self.nb + i // self.nc, rows, :], buf, self.asem.at[slot])

    def ocopy(self, b):
        sl = lax.rem(b, 2)
        up = pl.multiple_of(self.up_off + b * self.nb, self.nb)
        dn = pl.multiple_of(self.down_off + b * self.nb, self.nb)
        return (pltpu.make_async_copy(self.o1.at[sl], self.out_up.at[:, pl.ds(up, self.nb)], self.osem.at[0, sl]),
                pltpu.make_async_copy(self.o2.at[sl], self.out_down.at[pl.ds(dn, self.nb), :], self.osem.at[1, sl]))

    def ocopy(self, b):
        sl = lax.rem(b, 2)
        up = pl.multiple_of(self.up_off + b * self.nb, self.nb)
        dn = pl.multiple_of(self.down_off + b * self.nb, self.nb)
        return (pltpu.make_async_copy(self.o1.at[sl], self.out_up.at[:, pl.ds(up, self.nb)], self.osem.at[0, sl]),
                pltpu.make_async_copy(self.o2.at[sl], self.out_down.at[pl.ds(dn, self.nb), :], self.osem.at[1, sl]))

    def prefetch(self):
        for x in self.wcopy(0):
            x.start()
        self.acopy(0, self.aba, 0).start()

    def step(self, i, dst, src, pre):
        nb, tc, sub, D = self.nb, self.tc, self.sub, self.D
        c, sl = lax.rem(i, self.nc), lax.rem(i // self.nc, 2)
        j = i - 1
        jc, jl = lax.rem(j, self.nc), lax.rem(j // self.nc, 2)

        def first(k):
            base = pl.multiple_of(c * tc + k * sub, sub)
            a = pre[k * sub:(k + 1) * sub, :]
            du = jnp.dot(self.DH[pl.ds(base, sub), :], self.w2b[sl], preferred_element_type=f32)
            u, slope = gelu_both(a)
            dst[k * sub:(k + 1) * sub, :nb] = u.astype(bf16)
            dst[k * sub:(k + 1) * sub, nb:] = (du * slope).astype(bf16)

        def second(q):
            keep = jc > 0
            base = pl.multiple_of(jc * tc, tc)
            n = slice(q * 256, (q + 1) * 256)
            p2 = lax.dot_general(src[:, :nb], self.DH[pl.ds(base, tc), n], ROWS, preferred_element_type=f32)
            self.o2[jl, :, n] = jnp.where(keep, self.o2[jl, :, n], 0.0) + p2
            p1 = lax.dot_general(self.R[pl.ds(base, tc), n], src[:, nb:], ROWS, preferred_element_type=f32)
            self.o1[jl, n, :] = jnp.where(keep, self.o1[jl, n, :], 0.0) + p1
        q = 0
        for k in range(tc // sub):
            first(k)
            while src is not None and q < ((k + 1) * (D // 256)) // (tc // sub):
                second(q)
                q += 1

    def prime(self):
        for x in self.wcopy(0):
            x.start()
        self.acopy(0, self.aba, 0).start()
        self.acopy(1, self.abb, 1).start()

    def run(self, loads, between):
        n, nc = self.nblk * self.nc, self.nc
        if loads is not None:
            loads(0)
        for x in self.wcopy(0):
            x.wait()
        for x in self.wcopy(1):
            x.start()
        self.acopy(0, self.aba, 0).wait()
        self.step(0, self.uda, None, self.aba)

        def body(ii, _):
            i = 2 * ii + 1
            b, odd = i // nc, lax.rem(ii, nc // 2)
            between(ii)
            if loads is not None:
                @pl.when(ii < nc // 2)
                def _():
                    loads(i)

                    @pl.when(i + 1 < nc)
                    def _():
                        loads(i + 1)

            @pl.when(odd == 0)
            def _():
                @pl.when(b >= 1)
                def _():
                    for x in self.ocopy(b - 1):
                        x.start()

                @pl.when(b >= 2)
                def _():
                    for x in self.ocopy(b - 2):
                        x.wait()
            self.acopy(lax.min(i + 1, n - 1), self.aba, 0).start()
            self.acopy(i, self.abb, 1).wait()
            self.step(i, self.udb, self.uda, self.abb)

            @pl.when((odd == nc // 2 - 1) & (b + 1 < self.nblk))
            def _():
                for x in self.wcopy(b + 1):
                    x.wait()

                @pl.when(b + 2 < self.nblk)
                def _():
                    for x in self.wcopy(b + 2):
                        x.start()
            self.acopy(lax.min(i + 2, n - 1), self.abb, 1).start()
            self.acopy(lax.min(i + 1, n - 1), self.aba, 0).wait()
            self.step(i + 1, self.uda, self.udb, self.aba)
            return 0
        lax.fori_loop(0, n // 2, body, 0)
        self.acopy(n - 1, self.abb, 1).wait()
        for x in self.ocopy(self.nblk - 1):
            x.start()

    def drain(self):
        for b in (self.nblk - 2, self.nblk - 1):
            for x in self.ocopy(b):
                x.wait()


def sweep_scratch(T, D, nb, tc):
    dma = pltpu.SemaphoreType.DMA
    return [pltpu.VMEM((T, D), bf16), pltpu.VMEM((T, D), bf16), pltpu.VMEM((2, D, nb), bf16),
            pltpu.VMEM((2, D, nb), f32), pltpu.VMEM((2, nb, D), f32), pltpu.VMEM((tc, 2 * nb), bf16), pltpu.VMEM((tc, 2 * nb), bf16),
            pltpu.VMEM((tc, nb), f32), pltpu.VMEM((tc, nb), f32), dma((2,)), dma((2, 2)), dma((2,))]


def spread_call(T, D, FF, ny, nz, ns, nb, tc, sub, nblk, when):
    nc = T // tc
    n_loc = FF - ns * ny * nz

    def kernel(rg, dhg, ap, w1, wt2, ga, gb, lu, ld, R, DH, w2b, o1, o2, uda, udb, aba, abb, wsem, osem, asem,
               s1b, s2b, sb, sn, us, das, lsem, ssem, loc, snd, rcv):
        data = lax.axis_index("data")
        z = data // ny
        y = lax.rem(data, ny)

        def plane(zz, yy):
            return {"data": lax.rem(zz + nz, nz) * ny + lax.rem(yy + ny, ny)}

        yup, ydn, zup, zdn = plane(z, y + 1), plane(z, y - 1), plane(z + 1, y), plane(z - 1, y)
        start = pl.multiple_of(n_loc + data * ns, ns)
        sw = [pltpu.make_async_copy(w1.at[:, pl.ds(start, ns)], s1b, ssem.at[0]),
              pltpu.make_async_copy(wt2.at[:, pl.ds(start, ns)], s2b, ssem.at[1])]
        for x in sw:
            x.start()

        def token_copy(c):
            rows = pl.ds(pl.multiple_of(c * tc, tc), tc)
            return (pltpu.make_async_copy(rg.at[rows], R.at[rows], lsem.at[0, c]),
                    pltpu.make_async_copy(dhg.at[rows], DH.at[rows], lsem.at[1, c]))
        for c in range(nc):
            for x in token_copy(c):
                x.start()
        bar = pltpu.get_barrier_semaphore()
        for dev in (yup, ydn, zup, zdn):
            pl.semaphore_signal(bar, inc=1, device_id=dev, device_id_type=MESH)
        pl.semaphore_wait(bar, 4)
        sweep = Sweep(T, D, nb, tc, sub, nblk, 0, (R, DH, w2b, o1, o2, uda, udb, aba, abb, wsem, osem, asem), ap, wt2, lu, ld, 0, 0)
        sweep.prime()
        for x in sw:
            x.wait()

        def own(c, _):
            for x in token_copy(c):
                x.wait()
            base = pl.multiple_of(c * tc, tc)
            for k in range(tc // sub):
                at = pl.ds(pl.multiple_of(base + k * sub, sub), sub)
                a = jnp.dot(R[at, :], s1b[...], preferred_element_type=f32)
                du = jnp.dot(DH[at, :], s2b[...], preferred_element_type=f32)
                u, slope = gelu_both(a)
                us[at, :] = u.astype(bf16)
                das[at, :] = (du * slope).astype(bf16)
            return 0

        def at(p, zz, yy, half):
            buf, n = ((ga, D), (gb, ns))[p]
            return buf.at[zz, yy] if half is None else buf.at[zz, yy, pl.ds(half * (n // 2), n // 2), :]
        plan = ring_plan(z, y, nz, ny, lambda p: (sn, sb)[p], at)
        entry = {e[0]: e for group in plan for e in group}

        def copy(k):
            _, a, b, dev = entry[k]
            return pltpu.make_async_remote_copy(src_ref=a, dst_ref=b, send_sem=snd.at[k], recv_sem=rcv.at[k], device_id=dev, device_id_type=MESH)

        def act(g):
            for k in NEEDS[g]:
                copy(k).wait_recv()
            for e in plan[g]:
                copy(e[0]).start()
        keep_a = pltpu.make_async_copy(sn, ga.at[z, y], loc.at[0])
        keep_b = pltpu.make_async_copy(sb, gb.at[z, y], loc.at[1])
        lax.fori_loop(0, nc, own, 0)
        half = D // 3

        def down_half(k, _):
            at = pl.ds(pl.multiple_of(k * half, half), half)
            sb[:, at] = lax.dot_general(us[...], DH[:, at], ROWS, preferred_element_type=f32)
            return 0

        def up_half(k, _):
            at = pl.ds(pl.multiple_of(k * half, half), half)
            sn[at, :] = lax.dot_general(das[...], R[:, at], ROWS, preferred_element_type=f32).T
            return 0
        lax.fori_loop(0, 3, down_half, 0)
        for k in (2, 3):
            copy(k).start()
        keep_b.start()
        lax.fori_loop(0, 3, up_half, 0)
        for k in (0, 1, 4, 5, 6, 7):
            copy(k).start()
        keep_a.start()

        def between(ii):
            hit = ii == when[0]
            for t in when[1:]:
                hit = hit | (ii == t)

            @pl.when(hit)
            def _():
                for g, t in enumerate(when):
                    @pl.when(ii == t)
                    def _(g=g):
                        act(g + 1)
        sweep.run(None, between)
        for k in LAST_ONES:
            copy(k).wait_recv()
        for k in range(40):
            copy(k).wait_send()
        keep_a.wait()
        keep_b.wait()
        sweep.drain()

    dma = pltpu.SemaphoreType.DMA
    anyspec = pl.BlockSpec(memory_space=pl.ANY)
    S = jax.ShapeDtypeStruct
    return pl.pallas_call(
        kernel,
        in_specs=[anyspec] * 5,
        out_specs=[anyspec] * 4,
        out_shape=[S((nz, ny, D, ns), f32), S((nz, ny, ns, D), f32), S((D, nb * nblk), f32), S((nb * nblk, D), f32)],
        scratch_shapes=sweep_scratch(T, D, nb, tc) + [
            pltpu.VMEM((D, ns), bf16), pltpu.VMEM((D, ns), bf16), pltpu.VMEM((ns, D), f32), pltpu.VMEM((D, ns), f32),
            pltpu.VMEM((T, ns), bf16), pltpu.VMEM((T, ns), bf16), dma((2, nc)), dma((2,)), dma((2,)), dma((40,)), dma((40,))],
        compiler_params=pltpu.CompilerParams(collective_id=1, has_side_effects=True, vmem_limit_bytes=62 << 20),
        cost_estimate=pl.CostEstimate(flops=8 * nb * nblk * T * D, bytes_accessed=4 * T * D + 12 * nb * nblk * D, transcendentals=0),
        name="spread",
    )


def final_call(T, D, FF, n_dev, ns, nb, tc, sub, done):
    nc = T // tc
    n_loc = FF - ns * n_dev
    nblk = n_loc // nb - done
    n_sp = ns * n_dev
    pairs = nblk * nc // 2
    rows = ns
    tasks = done * nb // rows + n_dev
    per = -(-tasks // pairs)

    def kernel(rg, dhg, ap, wt2, ga, gb, lu, ld, up, down, R, DH, w2b, o1, o2, uda, udb, aba, abb, wsem, osem, asem,
               cu, cd, lsem, isem, tsem):
        def token_copy(c):
            r = pl.ds(pl.multiple_of(c * tc, tc), tc)
            return (pltpu.make_async_copy(rg.at[r], R.at[r], lsem.at[0, c]),
                    pltpu.make_async_copy(dhg.at[r], DH.at[r], lsem.at[1, c]))
        sweep = Sweep(T, D, nb, tc, sub, nblk, done * nb, (R, DH, w2b, o1, o2, uda, udb, aba, abb, wsem, osem, asem), ap, wt2, up, down,
                      done * nb, done * nb)
        sweep.prime()
        for c in range(nc):
            for x in token_copy(c):
                x.start()
        n_l = done * nb // rows

        def ins(t, k):
            lo = pl.multiple_of(lax.min(t, n_l - 1) * rows, rows)
            sp = lax.max(t - n_l, 0)
            return ([pltpu.make_async_copy(ld.at[pl.ds(lo, rows), :], cd.at[k], isem.at[0, k]),
                     pltpu.make_async_copy(lu.at[:, pl.ds(lo, rows)], cu.at[k], isem.at[1, k])],
                    [pltpu.make_async_copy(gb.at[sp], cd.at[k], isem.at[0, k]),
                     pltpu.make_async_copy(ga.at[sp], cu.at[k], isem.at[1, k])])

        def outs(t, k):
            at = pl.multiple_of(jnp.where(t < n_l, t * rows, n_loc + (t - n_l) * rows), rows)
            return [pltpu.make_async_copy(cd.at[k], down.at[pl.ds(at, rows), :], tsem.at[0, k]),
                    pltpu.make_async_copy(cu.at[k], up.at[:, pl.ds(at, rows)], tsem.at[1, k])]

        def loop(g, what):
            def one(k, _):
                t = g * per + k

                @pl.when((t >= 0) & (t < tasks))
                def _():
                    what(t, lax.rem(t + 2 * per, 2 * per))
                return 0
            lax.fori_loop(0, per, one, 0)

        def fetch(t, k):
            @pl.when(t < n_l)
            def _():
                for x in ins(t, k)[0]:
                    x.start(priority=1)

            @pl.when(t >= n_l)
            def _():
                for x in ins(t, k)[1]:
                    x.start(priority=1)

        def put(t, k):
            for x in ins(t, k)[0]:
                x.wait()
            for x in outs(t, k):
                x.start(priority=1)

        def settle(t, k):
            for x in outs(t, k):
                x.wait()

        def between(ii):
            loop(ii - 1, settle)
            loop(ii + 1, fetch)
            loop(ii, put)
        loop(0, fetch)
        sweep.run(lambda c: [x.wait() for x in token_copy(c)], between)
        loop(pairs - 1, settle)
        sweep.drain()

    dma = pltpu.SemaphoreType.DMA
    anyspec = pl.BlockSpec(memory_space=pl.ANY)
    S = jax.ShapeDtypeStruct
    return pl.pallas_call(
        kernel,
        in_specs=[anyspec] * 8,
        out_specs=[anyspec] * 2,
        out_shape=[S((D, FF), f32), S((FF, D), f32)],
        scratch_shapes=sweep_scratch(T, D, nb, tc) + [
            pltpu.VMEM((2 * per, D, rows), f32), pltpu.VMEM((2 * per, rows, D), f32),
            dma((2, nc)), dma((2, 2 * per)), dma((2, 2 * per))],
        compiler_params=pltpu.CompilerParams(vmem_limit_bytes=63 << 20),
        cost_estimate=pl.CostEstimate(flops=8 * nb * nblk * T * D, bytes_accessed=4 * T * D + 24 * FF * D, transcendentals=0),
        name="final",
    )


def solution(mesh):
    n_stage = mesh.shape["stage"]
    n_data = mesh.shape["data"]
    ny = int(round(n_data ** 0.5))
    nz = n_data // ny
    ns, nb, tc, sub, done = 128, 256, 1024, 256, 12
    when = (4, 7, 9, 15, 20)
    times = ((-99, -99, 0, 0, 0, 0, 0, 1, 1, 2, 2, 3), (0, 2, 2, 4, 4, 6, 8, 11, 14, 14, 17, 20), (0, 1, 1, 3, 3, 5, 7, 10, 12, 12, 15, 17), (0, 1, 1, 4, 4, 7, 9, 14, 17, 17, 21, 24))
    ahead = (28, 10, 12, 8)

    def local_step(x_in, y_tgt, w_up, w_down, gain):
        n_micro, T, D = x_in.shape
        FF = w_up.shape[2]
        w1, w2 = w_up[0], w_down[0]
        tok_total = n_data * n_micro * T
        n_pre = (FF - ns * n_data) // nb
        rg, dhg, _, wt2, ap, dg, loss = chain_call(T, D, FF, ny, nz, n_stage, tok_total, 256, 4, nb, tc, n_pre, times, ahead)(x_in, y_tgt, gain, w1, w2)
        rg = rg.reshape(tok_total, D)
        dhg = dhg.reshape(tok_total, D)
        ga, gb, lu, ld = spread_call(tok_total, D, FF, ny, nz, ns, nb, tc, sub, done, when)(rg, dhg, ap, w1, wt2)
        ga = ga.reshape(n_data, D, ns)
        gb = gb.reshape(n_data, ns, D)
        up, down = final_call(tok_total, D, FF, n_data, ns, nb, tc, sub, done)(rg, dhg, ap, wt2, ga, gb, lu, ld)
        return up[None], down[None], dg, loss[0, :1]

    return jax.shard_map(local_step, mesh=mesh, in_specs=(P(("part", "data"), None, None), P(("part", "data"), None, None), P("stage", None, None), P("stage", None, None), P("stage", None)), out_specs=(P(("part", "stage"), None, None), P(("part", "stage"), None, None), P(("part", "stage"), None), P("part")), check_vma=False)
```

```python
import functools
import math

import jax
import jax.numpy as jnp
from jax import lax
from jax.experimental import pallas as pl
from jax.experimental.pallas import tpu as pltpu
from jax.sharding import PartitionSpec as P

EPS = 1e-6
C0 = math.sqrt(2.0 / math.pi)
CUB = 0.044715
f32 = jnp.float32
bf16 = jnp.bfloat16
MESH = pl.DeviceIdType.MESH
ROWS = (((0,), (0,)), ((), ()))
LASTS = (((1,), (1,)), ((), ()))


def gelu_u(a):
    t = jnp.tanh(C0 * (a + CUB * (a * a * a)))
    return a * (0.5 * (1.0 + t))


def gelu_both(a):
    a2 = a * a
    t = jnp.tanh(C0 * (a + CUB * (a2 * a)))
    half = 0.5 * (1.0 + t)
    slope = half + (0.5 * a) * (1.0 - t * t) * (C0 + (3.0 * CUB * C0) * a2)
    return a * half, slope


def inv_rms(x):
    return lax.rsqrt(jnp.mean(x * x, axis=-1, keepdims=True) + EPS)


NEEDS = ((), (0, 1, 2, 3), (4, 5, 6, 7), (8, 9, 10, 11), (12, 13, 14, 15, 16, 17, 18, 19), (24, 25, 26, 27))
LAST_ONES = tuple(range(20, 24)) + tuple(range(28, 40))


def ring_plan(z, y, nz, ny, mine, at):
    def plane(zz, yy):
        return {"data": lax.rem(zz + nz, nz) * ny + lax.rem(yy + ny, ny)}

    up = (plane(z, y + 1), plane(z + 1, y))
    dn = (plane(z, y - 1), plane(z - 1, y))
    plus = (lambda k: (z, lax.rem(y + k + ny, ny)), lambda k: (lax.rem(z + k + nz, nz), y))

    def cross(p, j, k):
        zz, yy = lax.rem(z + nz + (k if p == 0 else j), nz), lax.rem(y + ny + (j if p == 0 else k), ny)
        return (p, zz, yy)

    groups = []
    groups.append([(2 * p + d, mine(p), at(p, z, y, None), (up, dn)[d][p]) for p in (0, 1) for d in (0, 1)]
                  + [(4 + 2 * p + d, mine(p), at(p, z, y, None), (up, dn)[d][1 - p]) for p in (0, 1) for d in (0, 1)])

    def thru(k, where, half, dev):
        ref = at(*where, half)
        return (k, ref, ref, dev)
    g = [thru(8 + 2 * p + d, cross(p, (-1, 1)[d], 0), d, (up, dn)[d][p]) for p in (0, 1) for d in (0, 1)]
    g += [thru(12 + 4 * p + 2 * j + d, cross(p, (-1, 1)[j], 0), None, (up, dn)[d][1 - p]) for p in (0, 1) for j in (0, 1) for d in (0, 1)]
    groups.append(g)
    groups.append([thru(20 + 2 * p + d, cross(p, 0, (-1, 1)[d]), d, (up, dn)[d][1 - p]) for p in (0, 1) for d in (0, 1)])
    groups.append([thru(24 + 2 * p + d, cross(p, 2, 0), None, (up, dn)[d][1 - p]) for p in (0, 1) for d in (0, 1)])
    groups.append([thru(28 + 4 * p + 2 * j + d, cross(p, (-1, 1)[j], (-1, 1)[d]), d, (up, dn)[d][1 - p])
                   for p in (0, 1) for j in (0, 1) for d in (0, 1)])
    groups.append([thru(36 + 2 * p + d, cross(p, 2, (-1, 1)[d]), d, (up, dn)[d][1 - p]) for p in (0, 1) for d in (0, 1)])
    return groups


def chain_call(T, D, FF, ny, nz, n_stage, tok_total, cb, nj, nb, tc, n_pre, times, ahead):
    cw = FF // nj
    last = n_stage - 1
    h = T // 2
    qr = T // 4
    early = (n_stage * 3) // 8

    nc = tok_total // tc
    n_turn = n_pre // 2 * nc

    def kernel(x_ref, y_ref, g_ref, w1, w2, rg, dhg, wt1, wt2, ap, dg_o, loss_o,
               pbuf, qbuf, a_s, acc, xb, ob, rb, db, dxb, ts1, ts2, ast, lossb, exy, exz, dgacc,
               wsem, tsem1, tsem2, xs, xr, ds, dr_, ls, lr, ags, agr, own, exs, exr, rsem, asem):
        data = lax.axis_index("data")
        s = lax.axis_index("stage")
        z = data // ny
        y = lax.rem(data, ny)

        def plane(zz, yy):
            return {"data": lax.rem(zz + nz, nz) * ny + lax.rem(yy + ny, ny)}

        yp, ym = lax.rem(y + 1, ny), lax.rem(y + ny - 1, ny)
        zp, zm = lax.rem(z + 1, nz), lax.rem(z + nz - 1, nz)
        nxt = {"stage": lax.rem(s + 1, n_stage)}
        prv = {"stage": lax.rem(s + n_stage - 1, n_stage)}

        def part(j):
            return pl.ds(pl.multiple_of(j * cw, cw), cw)

        def weights(src_p, src_q, j):
            return (pltpu.make_async_copy(src_p.at[:, part(j)], pbuf.at[:, part(j)], wsem.at[0, j]),
                    pltpu.make_async_copy(src_q.at[part(j), :], qbuf.at[part(j), :], wsem.at[1, j]))

        def each_weight(src_p, src_q, what):
            def one(j, _):
                for x in weights(src_p, src_q, j):
                    getattr(x, what)()
                return 0
            lax.fori_loop(0, nj, one, 0)
        each_weight(w1, w2, "start")

        bar = pltpu.get_barrier_semaphore()
        for dev in [plane(z, y + k) for k in range(1, ny)] + [plane(z + k, y) for k in range(1, nz)] + [nxt, prv]:
            pl.semaphore_signal(bar, inc=1, device_id=dev, device_id_type=MESH)
        pl.semaphore_wait(bar, ny + nz)

        def rc(src, dst, ssem, rsem, dev):
            return pltpu.make_async_remote_copy(src_ref=src, dst_ref=dst, send_sem=ssem, recv_sem=rsem, device_id=dev, device_id_type=MESH)

        def ag(t, m, src, dst):
            def at(p, zz, yy, half):
                rows = pl.ds(p * h, h) if half is None else pl.ds(p * h + half * qr, qr)
                return dst.at[zz, yy, m, rows]
            groups = ring_plan(z, y, nz, ny, lambda p: src.at[m, pl.ds(p * h, h)], at)
            entry = {e[0]: e for group in groups for e in group}

            def copy(k):
                _, a, b, dev = entry[k]
                return rc(a, b, ags.at[t, m, k], agr.at[t, m, k], dev)

            def start(g):
                for k in NEEDS[g]:
                    copy(k).wait_recv()
                for e in groups[g]:
                    copy(e[0]).start()
                if g == 0:
                    pltpu.make_async_copy(src.at[m], dst.at[z, y, m], own.at[t, m]).start()

            def finish():
                for k in LAST_ONES:
                    copy(k).wait_recv()
                for k in range(40):
                    copy(k).wait_send()
                pltpu.make_async_copy(src.at[m], dst.at[z, y, m], own.at[t, m]).wait()
            return start, finish

        def ag_start(t, m, src, dst):
            ag(t, m, src, dst)[0](0)

        def ag_half(t, src, dst):
            for g in (1, 2, 3):
                for m in range(2):
                    ag(t, m, src, dst)[0](g)

        def ag_tail(t, src, dst):
            for g in (4, 5):
                for m in range(2):
                    ag(t, m, src, dst)[0](g)
            for m in range(2):
                ag(t, m, src, dst)[1]()

        def transposes():
            nb = FF // cb

            def cp1(c, slot):
                return pltpu.make_async_copy(ts1.at[slot], wt1.at[pl.ds(c * cb, cb), :], tsem1.at[slot])

            def cp2(c, slot):
                return pltpu.make_async_copy(ts2.at[slot], wt2.at[:, pl.ds(c * cb, cb)], tsem2.at[slot])

            def body(c, _):
                slot = lax.rem(c, 2)

                @pl.when(c >= 2)
                def _():
                    cp1(c - 2, slot).wait()
                    cp2(c - 2, slot).wait()
                off = pl.multiple_of(c * cb, cb)
                ts1[slot] = pbuf[:, pl.ds(off, cb)].T
                ts2[slot] = qbuf[pl.ds(off, cb), :].T
                cp1(c, slot).start()
                cp2(c, slot).start()
                return 0
            lax.fori_loop(0, nb, body, 0)
            for c in (nb - 2, nb - 1):
                cp1(c, c % 2).wait()
                cp2(c, c % 2).wait()

        gain = g_ref[...]

        def two_dots(first, slow, src_p, src_q):
            @pl.when(slow)
            def _():
                def one(j, _):
                    for x in weights(src_p, src_q, j):
                        x.wait()
                    p = jnp.dot(first(j), qbuf[part(j), :], preferred_element_type=f32)
                    acc[...] = jnp.where(j > 0, acc[...], 0.0) + p
                    return 0
                lax.fori_loop(0, nj, one, 0)

            @pl.when(jnp.logical_not(slow))
            def _():
                fast_dots(first)

        def fast_dots(first):
            def second(j, u):
                p = jnp.dot(u, qbuf[j * cw:(j + 1) * cw, :], preferred_element_type=f32)
                if j == 0:
                    acc[...] = p
                else:
                    acc[...] += p
            u = first(0)
            for j in range(1, nj):
                un = first(j)
                second(j - 1, u)
                u = un
            second(nj - 1, u)

        @pl.when(s == 0)
        def _():
            xb[...] = x_ref[...]
        lossb[...] = jnp.zeros_like(lossb)

        @pl.when(s > 0)
        def _():
            each_weight(w1, w2, "wait")

        @pl.when(s >= early)
        def _():
            transposes()

        def x_send(m):
            return rc(ob.at[m], xb.at[m], xs.at[m], xr.at[m], nxt)

        def fwd(m, _):
            @pl.when(s > 0)
            def _():
                x_send(m).wait_recv()
            x = xb[m].astype(f32)
            r = (x * inv_rms(x) * gain).astype(bf16)
            rb[m] = r
            ag_start(0, m, rb, rg)

            def first(j):
                a = jnp.dot(rb[m], pbuf[:, part(j)], preferred_element_type=f32)
                a_s[m, :, part(j)] = a
                return gelu_u(a).astype(bf16)
            two_dots(first, (s == 0) & (m == 0), w1, w2)
            ob[m] = (xb[m].astype(f32) + acc[...]).astype(bf16)

            @pl.when(s < last)
            def _():
                x_send(m).start()

            @pl.when(s == last)
            def _():
                e = ob[m].astype(f32) - y_ref[m].astype(f32)
                lossb[...] += jnp.sum(e * e)
                db[m] = (e * (1.0 / tok_total)).astype(bf16)
            return 0
        lax.fori_loop(0, 2, fwd, 0)

        @pl.when(s < early)
        def _():
            transposes()
        @pl.when(s >= n_stage // 2)
        def _():
            each_weight(wt2, wt1, "start")

        def r_copy(i):
            dev, m = i // 2, lax.rem(i, 2)
            return pltpu.make_async_copy(rg.at[dev // ny, lax.rem(dev, ny), m], qbuf.at[pl.ds(pl.multiple_of(i * T, T), T), :], rsem.at[i])

        def r_start(i, _):
            r_copy(i).start()
            return 0

        def r_wait(i, _):
            r_copy(i).wait()
            return 0

        def a_copies(i):
            slot, pair = lax.rem(i, 2), i // nc
            rows = pl.ds(pl.multiple_of(lax.rem(i, nc) * tc, tc), tc)
            return [pltpu.make_async_copy(ast.at[slot, k], ap.at[2 * pair + k, rows, :], asem.at[slot, k]) for k in range(2)]

        def turns(lo, hi, tick, whole):
            def turn(i, _):
                tick(i)

                @pl.when(i >= lo + 2)
                def _():
                    for c in a_copies(i - 2):
                        c.wait()
                slot, pair = lax.rem(i, 2), i // nc
                base = pl.multiple_of(lax.rem(i, nc) * tc, tc)

                def block(k, _):
                    cols = pl.ds(pl.multiple_of((2 * pair + k) * nb, nb), nb)
                    ast[slot, k] = jnp.dot(qbuf[pl.ds(base, tc), :], pbuf[:, cols], preferred_element_type=f32)
                    return 0
                if whole:
                    block(0, 0)
                    block(1, 0)
                else:
                    lax.fori_loop(0, 2, block, 0)
                for c in a_copies(i):
                    c.start()
                return 0
            lax.fori_loop(lo, hi, turn, 0)

            @pl.when(hi >= lo + 2)
            def _():
                for c in a_copies(hi - 2) + a_copies(hi - 1):
                    c.wait()
        n_early = jnp.where(s == 0, ahead[0], jnp.where(s == 1, ahead[1], jnp.where(s == 2, ahead[2], jnp.where(s == 3, ahead[3], 0))))

        l_send = rc(lossb, lossb, ls, lr, prv)

        @pl.when(s == last)
        def _():
            l_send.start()

        @pl.when(s < last)
        def _():
            ag_half(0, rb, rg)

        @pl.when(s < n_stage // 2)
        def _():
            ag_tail(0, rb, rg)
            lax.fori_loop(0, 2 * ny * nz, r_start, 0)
            lax.fori_loop(0, 2 * ny * nz, r_wait, 0)
            turns(0, n_early, lambda i: None, False)
            each_weight(wt2, wt1, "start")

        @pl.when(s < last)
        def _():
            each_weight(wt2, wt1, "wait")

        def d_send(m):
            return rc(dxb.at[m], db.at[m], ds.at[m], dr_.at[m], prv)

        dgacc[...] = jnp.zeros_like(dgacc)

        @pl.when(s == 0)
        def _():
            for m in range(2):
                d_send(m).wait_recv()
                ag_start(1, m, db, dhg)
            for m in range(2):
                ag(1, m, db, dhg)[0](1)

        def bwd(m, _):
            @pl.when((s < last) & (s > 0))
            def _():
                d_send(m).wait_recv()

            @pl.when(s > 0)
            def _():
                ag_start(1, m, db, dhg)

            def first(j):
                du = jnp.dot(db[m], pbuf[:, part(j)], preferred_element_type=f32)
                _, slope = gelu_both(a_s[m, :, part(j)])
                return (du * slope).astype(bf16)
            two_dots(first, (s == last) & (m == 0), wt2, wt1)
            x = xb[m].astype(f32)
            q = inv_rms(x)
            n = x * q
            dr = acc[...]
            dn = dr * gain
            dx = q * (dn - n * jnp.mean(dn * n, axis=-1, keepdims=True))
            dxb[m] = (db[m].astype(f32) + dx).astype(bf16)

            @pl.when(s > 0)
            def _():
                d_send(m).start()
            dgacc[...] += jnp.sum(dr * n, axis=0, keepdims=True)
            return 0
        lax.fori_loop(0, 2, bwd, 0)

        @pl.when(s < last)
        def _():
            l_send.wait_recv()

            @pl.when(s > 0)
            def _():
                l_send.start()

        exy[y, :, :D] = jnp.broadcast_to(dgacc[...], (8, D))
        exy[y, :, D:] = lossb[...]

        def ex(axis, k):
            buf, i, dev = (exy, y, plane(z, y + k)) if axis == 0 else (exz, z, plane(z + k, y))
            return rc(buf.at[i], buf.at[i], exs.at[axis, k - 1], exr.at[axis, k - 1], dev)
        for k in range(1, ny):
            ex(0, k).start()
        cw1 = pltpu.make_async_copy(w1, pbuf, wsem.at[0, 0])
        cw1.start()

        @pl.when(s == last)
        def _():
            ag_half(0, rb, rg)

        @pl.when(s >= n_stage // 2)
        def _():
            ag_tail(0, rb, rg)

        lax.fori_loop(0, 2 * ny * nz, r_start, 0)
        lax.fori_loop(0, 2 * ny * nz, r_wait, 0)
        cw1.wait()

        def ex_mid():
            for k in range(1, ny):
                ex(0, k).wait_recv()
            tot = exy[0]
            for k in range(1, ny):
                tot = tot + exy[k]
            exz[z] = tot
            for k in range(1, nz):
                ex(1, k).start()

        def ex_last():
            for k in range(1, nz):
                ex(1, k).wait_recv()
            tot = exz[0]
            for k in range(1, nz):
                tot = tot + exz[k]
            dg_o[...] = tot[0:1, :D]
            loss_o[...] = tot[0:1, D:] * (1.0 / (tok_total * D))

        def later(g, m):
            return lambda: ag(1, m, db, dhg)[0](g)
        events = [later(1, 0), later(1, 1), ex_mid, later(2, 0), later(2, 1), later(3, 0), later(3, 1), later(4, 0), later(4, 1),
                  ex_last, later(5, 0), later(5, 1)]
        due = [n_early + jnp.where(s == 0, t0, jnp.where(s == 1, t1, jnp.where(s < n_stage // 2, t2, t3))) for t0, t1, t2, t3 in zip(*times)]

        def tick(i):
            for t, event in zip(due, events):
                @pl.when(i == t)
                def _(event=event):
                    event()
        turns(n_early, n_turn, tick, True)
        for m in range(2):
            ag(1, m, db, dhg)[1]()
        for axis, n in ((0, ny), (1, nz)):
            for k in range(1, n):
                ex(axis, k).wait_send()

        @pl.when(s < last)
        def _():
            x_send(0).wait_send()
            x_send(1).wait_send()

        @pl.when(s > 0)
        def _():
            d_send(0).wait_send()
            d_send(1).wait_send()
            l_send.wait_send()

    dma = pltpu.SemaphoreType.DMA
    anyspec = pl.BlockSpec(memory_space=pl.ANY)
    vspec = pl.BlockSpec(memory_space=pltpu.VMEM)
    S = jax.ShapeDtypeStruct
    return pl.pallas_call(
        kernel,
        in_specs=[vspec, vspec, vspec, anyspec, anyspec],
        out_specs=[anyspec, anyspec, anyspec, anyspec, anyspec, vspec, vspec],
        out_shape=[S((nz, ny, 2, T, D), bf16), S((nz, ny, 2, T, D), bf16), S((FF, D), bf16), S((D, FF), bf16),
                   S((n_pre, tok_total, nb), f32), S((1, D), f32), S((1, 128), f32)],
        scratch_shapes=[
            pltpu.VMEM((D, FF), bf16), pltpu.VMEM((FF, D), bf16), pltpu.VMEM((2, T, FF), f32), pltpu.VMEM((T, D), f32),
            pltpu.VMEM((2, T, D), bf16), pltpu.VMEM((2, T, D), bf16), pltpu.VMEM((2, T, D), bf16),
            pltpu.VMEM((2, T, D), bf16), pltpu.VMEM((2, T, D), bf16),
            pltpu.VMEM((2, cb, D), bf16), pltpu.VMEM((2, D, cb), bf16), pltpu.VMEM((2, 2, tc, nb), f32),
            pltpu.VMEM((8, 128), f32), pltpu.VMEM((ny, 8, D + 128), f32), pltpu.VMEM((nz, 8, D + 128), f32),
            pltpu.VMEM((1, D), f32),
            dma((2, nj)), dma((2,)), dma((2,)), dma((2,)), dma((2,)), dma((2,)), dma((2,)), dma, dma,
            dma((2, 2, 40)), dma((2, 2, 40)), dma((2, 2)), dma((2, 3)), dma((2, 3)), dma((2 * ny * nz,)), dma((2, 2))],
        compiler_params=pltpu.CompilerParams(collective_id=0, has_side_effects=True, vmem_limit_bytes=63 << 20),
        cost_estimate=pl.CostEstimate(flops=8 * 2 * T * D * FF * 2, bytes_accessed=6 * D * FF * 2, transcendentals=0),
        name="chain",
    )


class Sweep:
    def __init__(self, T, D, nb, tc, sub, nblk, off, refs, ap, wt2, out_up, out_down, up_off, down_off):
        self.T, self.D, self.nb, self.tc, self.sub, self.nblk = T, D, nb, tc, sub, nblk
        self.off, self.up_off, self.down_off = off, up_off, down_off
        self.nc = T // tc
        self.ap, self.wt2, self.out_up, self.out_down = ap, wt2, out_up, out_down
        self.R, self.DH, self.w2b, self.o1, self.o2, self.uda, self.udb, self.aba, self.abb, self.wsem, self.osem, self.asem = refs

    def wcopy(self, b):
        sl = lax.rem(b, 2)
        at = pl.multiple_of(self.off + b * self.nb, self.nb)
        return (pltpu.make_async_copy(self.wt2.at[:, pl.ds(at, self.nb)], self.w2b.at[sl], self.wsem.at[sl]),)

    def acopy(self, i, buf, slot):
        rows = pl.ds(pl.multiple_of(lax.rem(i, self.nc) * self.tc, self.tc), self.tc)
        return pltpu.make_async_copy(self.ap.at[self.off // self.nb + i // self.nc, rows, :], buf, self.asem.at[slot])

    def ocopy(self, b):
        sl = lax.rem(b, 2)
        up = pl.multiple_of(self.up_off + b * self.nb, self.nb)
        dn = pl.multiple_of(self.down_off + b * self.nb, self.nb)
        return (pltpu.make_async_copy(self.o1.at[sl], self.out_up.at[:, pl.ds(up, self.nb)], self.osem.at[0, sl]),
                pltpu.make_async_copy(self.o2.at[sl], self.out_down.at[pl.ds(dn, self.nb), :], self.osem.at[1, sl]))

    def ocopy(self, b):
        sl = lax.rem(b, 2)
        up = pl.multiple_of(self.up_off + b * self.nb, self.nb)
        dn = pl.multiple_of(self.down_off + b * self.nb, self.nb)
        return (pltpu.make_async_copy(self.o1.at[sl], self.out_up.at[:, pl.ds(up, self.nb)], self.osem.at[0, sl]),
                pltpu.make_async_copy(self.o2.at[sl], self.out_down.at[pl.ds(dn, self.nb), :], self.osem.at[1, sl]))

    def prefetch(self):
        for x in self.wcopy(0):
            x.start()
        self.acopy(0, self.aba, 0).start()

    def step(self, i, dst, src, pre):
        nb, tc, sub, D = self.nb, self.tc, self.sub, self.D
        c, sl = lax.rem(i, self.nc), lax.rem(i // self.nc, 2)
        j = i - 1
        jc, jl = lax.rem(j, self.nc), lax.rem(j // self.nc, 2)

        def first(k):
            base = pl.multiple_of(c * tc + k * sub, sub)
            a = pre[k * sub:(k + 1) * sub, :]
            du = jnp.dot(self.DH[pl.ds(base, sub), :], self.w2b[sl], preferred_element_type=f32)
            u, slope = gelu_both(a)
            dst[k * sub:(k + 1) * sub, :nb] = u.astype(bf16)
            dst[k * sub:(k + 1) * sub, nb:] = (du * slope).astype(bf16)

        def second(q):
            keep = jc > 0
            base = pl.multiple_of(jc * tc, tc)
            n = slice(q * 256, (q + 1) * 256)
            p2 = lax.dot_general(src[:, :nb], self.DH[pl.ds(base, tc), n], ROWS, preferred_element_type=f32)
            self.o2[jl, :, n] = jnp.where(keep, self.o2[jl, :, n], 0.0) + p2
            p1 = lax.dot_general(self.R[pl.ds(base, tc), n], src[:, nb:], ROWS, preferred_element_type=f32)
            self.o1[jl, n, :] = jnp.where(keep, self.o1[jl, n, :], 0.0) + p1
        q = 0
        for k in range(tc // sub):
            first(k)
            while src is not None and q < ((k + 1) * (D // 256)) // (tc // sub):
                second(q)
                q += 1

    def prime(self):
        for x in self.wcopy(0):
            x.start()
        self.acopy(0, self.aba, 0).start()
        self.acopy(1, self.abb, 1).start()

    def run(self, loads, between):
        n, nc = self.nblk * self.nc, self.nc
        if loads is not None:
            loads(0)
        for x in self.wcopy(0):
            x.wait()
        for x in self.wcopy(1):
            x.start()
        self.acopy(0, self.aba, 0).wait()
        self.step(0, self.uda, None, self.aba)

        def body(ii, _):
            i = 2 * ii + 1
            b, odd = i // nc, lax.rem(ii, nc // 2)
            between(ii)
            if loads is not None:
                @pl.when(ii < nc // 2)
                def _():
                    loads(i)

                    @pl.when(i + 1 < nc)
                    def _():
                        loads(i + 1)

            @pl.when(odd == 0)
            def _():
                @pl.when(b >= 1)
                def _():
                    for x in self.ocopy(b - 1):
                        x.start()

                @pl.when(b >= 2)
                def _():
                    for x in self.ocopy(b - 2):
                        x.wait()
            self.acopy(lax.min(i + 1, n - 1), self.aba, 0).start()
            self.acopy(i, self.abb, 1).wait()
            self.step(i, self.udb, self.uda, self.abb)

            @pl.when((odd == nc // 2 - 1) & (b + 1 < self.nblk))
            def _():
                for x in self.wcopy(b + 1):
                    x.wait()

                @pl.when(b + 2 < self.nblk)
                def _():
                    for x in self.wcopy(b + 2):
                        x.start()
            self.acopy(lax.min(i + 2, n - 1), self.abb, 1).start()
            self.acopy(lax.min(i + 1, n - 1), self.aba, 0).wait()
            self.step(i + 1, self.uda, self.udb, self.aba)
            return 0
        lax.fori_loop(0, n // 2, body, 0)
        self.acopy(n - 1, self.abb, 1).wait()
        for x in self.ocopy(self.nblk - 1):
            x.start()

    def drain(self):
        for b in (self.nblk - 2, self.nblk - 1):
            for x in self.ocopy(b):
                x.wait()


def sweep_scratch(T, D, nb, tc):
    dma = pltpu.SemaphoreType.DMA
    return [pltpu.VMEM((T, D), bf16), pltpu.VMEM((T, D), bf16), pltpu.VMEM((2, D, nb), bf16),
            pltpu.VMEM((2, D, nb), f32), pltpu.VMEM((2, nb, D), f32), pltpu.VMEM((tc, 2 * nb), bf16), pltpu.VMEM((tc, 2 * nb), bf16),
            pltpu.VMEM((tc, nb), f32), pltpu.VMEM((tc, nb), f32), dma((2,)), dma((2, 2)), dma((2,))]


def spread_call(T, D, FF, ny, nz, ns, nb, tc, sub, nblk, when):
    nc = T // tc
    n_loc = FF - ns * ny * nz

    def kernel(rg, dhg, ap, w1, wt2, ga, gb, lu, ld, R, DH, w2b, o1, o2, uda, udb, aba, abb, wsem, osem, asem,
               s1b, s2b, sb, sn, us, das, lsem, ssem, loc, snd, rcv):
        data = lax.axis_index("data")
        z = data // ny
        y = lax.rem(data, ny)

        def plane(zz, yy):
            return {"data": lax.rem(zz + nz, nz) * ny + lax.rem(yy + ny, ny)}

        yup, ydn, zup, zdn = plane(z, y + 1), plane(z, y - 1), plane(z + 1, y), plane(z - 1, y)
        start = pl.multiple_of(n_loc + data * ns, ns)
        sw = [pltpu.make_async_copy(w1.at[:, pl.ds(start, ns)], s1b, ssem.at[0]),
              pltpu.make_async_copy(wt2.at[:, pl.ds(start, ns)], s2b, ssem.at[1])]
        for x in sw:
            x.start()

        def token_copy(c):
            rows = pl.ds(pl.multiple_of(c * tc, tc), tc)
            return (pltpu.make_async_copy(rg.at[rows], R.at[rows], lsem.at[0, c]),
                    pltpu.make_async_copy(dhg.at[rows], DH.at[rows], lsem.at[1, c]))
        for c in range(nc):
            for x in token_copy(c):
                x.start()
        bar = pltpu.get_barrier_semaphore()
        for dev in (yup, ydn, zup, zdn):
            pl.semaphore_signal(bar, inc=1, device_id=dev, device_id_type=MESH)
        pl.semaphore_wait(bar, 4)
        sweep = Sweep(T, D, nb, tc, sub, nblk, 0, (R, DH, w2b, o1, o2, uda, udb, aba, abb, wsem, osem, asem), ap, wt2, lu, ld, 0, 0)
        sweep.prime()
        for x in sw:
            x.wait()

        def own(c, _):
            for x in token_copy(c):
                x.wait()
            base = pl.multiple_of(c * tc, tc)
            for k in range(tc // sub):
                at = pl.ds(pl.multiple_of(base + k * sub, sub), sub)
                a = jnp.dot(R[at, :], s1b[...], preferred_element_type=f32)
                du = jnp.dot(DH[at, :], s2b[...], preferred_element_type=f32)
                u, slope = gelu_both(a)
                us[at, :] = u.astype(bf16)
                das[at, :] = (du * slope).astype(bf16)
            return 0

        def at(p, zz, yy, half):
            buf, n = ((ga, D), (gb, ns))[p]
            return buf.at[zz, yy] if half is None else buf.at[zz, yy, pl.ds(half * (n // 2), n // 2), :]
        plan = ring_plan(z, y, nz, ny, lambda p: (sn, sb)[p], at)
        entry = {e[0]: e for group in plan for e in group}

        def copy(k):
            _, a, b, dev = entry[k]
            return pltpu.make_async_remote_copy(src_ref=a, dst_ref=b, send_sem=snd.at[k], recv_sem=rcv.at[k], device_id=dev, device_id_type=MESH)

        def act(g):
            for k in NEEDS[g]:
                copy(k).wait_recv()
            for e in plan[g]:
                copy(e[0]).start()
        keep_a = pltpu.make_async_copy(sn, ga.at[z, y], loc.at[0])
        keep_b = pltpu.make_async_copy(sb, gb.at[z, y], loc.at[1])
        lax.fori_loop(0, nc, own, 0)
        half = D // 3

        def down_half(k, _):
            at = pl.ds(pl.multiple_of(k * half, half), half)
            sb[:, at] = lax.dot_general(us[...], DH[:, at], ROWS, preferred_element_type=f32)
            return 0

        def up_half(k, _):
            at = pl.ds(pl.multiple_of(k * half, half), half)
            sn[at, :] = lax.dot_general(das[...], R[:, at], ROWS, preferred_element_type=f32).T
            return 0
        lax.fori_loop(0, 3, down_half, 0)
        for k in (2, 3):
            copy(k).start()
        keep_b.start()
        lax.fori_loop(0, 3, up_half, 0)
        for k in (0, 1, 4, 5, 6, 7):
            copy(k).start()
        keep_a.start()

        def between(ii):
            hit = ii == when[0]
            for t in when[1:]:
                hit = hit | (ii == t)

            @pl.when(hit)
            def _():
                for g, t in enumerate(when):
                    @pl.when(ii == t)
                    def _(g=g):
                        act(g + 1)
        sweep.run(None, between)
        for k in LAST_ONES:
            copy(k).wait_recv()
        for k in range(40):
            copy(k).wait_send()
        keep_a.wait()
        keep_b.wait()
        sweep.drain()

    dma = pltpu.SemaphoreType.DMA
    anyspec = pl.BlockSpec(memory_space=pl.ANY)
    S = jax.ShapeDtypeStruct
    return pl.pallas_call(
        kernel,
        in_specs=[anyspec] * 5,
        out_specs=[anyspec] * 4,
        out_shape=[S((nz, ny, D, ns), f32), S((nz, ny, ns, D), f32), S((D, nb * nblk), f32), S((nb * nblk, D), f32)],
        scratch_shapes=sweep_scratch(T, D, nb, tc) + [
            pltpu.VMEM((D, ns), bf16), pltpu.VMEM((D, ns), bf16), pltpu.VMEM((ns, D), f32), pltpu.VMEM((D, ns), f32),
            pltpu.VMEM((T, ns), bf16), pltpu.VMEM((T, ns), bf16), dma((2, nc)), dma((2,)), dma((2,)), dma((40,)), dma((40,))],
        compiler_params=pltpu.CompilerParams(collective_id=1, has_side_effects=True, vmem_limit_bytes=62 << 20),
        cost_estimate=pl.CostEstimate(flops=8 * nb * nblk * T * D, bytes_accessed=4 * T * D + 12 * nb * nblk * D, transcendentals=0),
        name="spread",
    )


def final_call(T, D, FF, n_dev, ns, nb, tc, sub, done):
    nc = T // tc
    n_loc = FF - ns * n_dev
    nblk = n_loc // nb - done
    n_sp = ns * n_dev
    pairs = nblk * nc // 2
    rows = ns
    tasks = done * nb // rows + n_dev
    per = -(-tasks // pairs)

    def kernel(rg, dhg, ap, wt2, ga, gb, lu, ld, up, down, R, DH, w2b, o1, o2, uda, udb, aba, abb, wsem, osem, asem,
               cu, cd, lsem, isem, tsem):
        def token_copy(c):
            r = pl.ds(pl.multiple_of(c * tc, tc), tc)
            return (pltpu.make_async_copy(rg.at[r], R.at[r], lsem.at[0, c]),
                    pltpu.make_async_copy(dhg.at[r], DH.at[r], lsem.at[1, c]))
        sweep = Sweep(T, D, nb, tc, sub, nblk, done * nb, (R, DH, w2b, o1, o2, uda, udb, aba, abb, wsem, osem, asem), ap, wt2, up, down,
                      done * nb, done * nb)
        sweep.prime()
        for c in range(nc):
            for x in token_copy(c):
                x.start()
        n_l = done * nb // rows

        def ins(t, k):
            lo = pl.multiple_of(lax.min(t, n_l - 1) * rows, rows)
            sp = lax.max(t - n_l, 0)
            return ([pltpu.make_async_copy(ld.at[pl.ds(lo, rows), :], cd.at[k], isem.at[0, k]),
                     pltpu.make_async_copy(lu.at[:, pl.ds(lo, rows)], cu.at[k], isem.at[1, k])],
                    [pltpu.make_async_copy(gb.at[sp], cd.at[k], isem.at[0, k]),
                     pltpu.make_async_copy(ga.at[sp], cu.at[k], isem.at[1, k])])

        def outs(t, k):
            at = pl.multiple_of(jnp.where(t < n_l, t * rows, n_loc + (t - n_l) * rows), rows)
            return [pltpu.make_async_copy(cd.at[k], down.at[pl.ds(at, rows), :], tsem.at[0, k]),
                    pltpu.make_async_copy(cu.at[k], up.at[:, pl.ds(at, rows)], tsem.at[1, k])]

        def loop(g, what):
            def one(k, _):
                t = g * per + k

                @pl.when((t >= 0) & (t < tasks))
                def _():
                    what(t, lax.rem(t + 2 * per, 2 * per))
                return 0
            lax.fori_loop(0, per, one, 0)

        def fetch(t, k):
            @pl.when(t < n_l)
            def _():
                for x in ins(t, k)[0]:
                    x.start(priority=1)

            @pl.when(t >= n_l)
            def _():
                for x in ins(t, k)[1]:
                    x.start(priority=1)

        def put(t, k):
            for x in ins(t, k)[0]:
                x.wait()
            for x in outs(t, k):
                x.start(priority=1)

        def settle(t, k):
            for x in outs(t, k):
                x.wait()

        def between(ii):
            loop(ii - 1, settle)
            loop(ii + 1, fetch)
            loop(ii, put)
        loop(0, fetch)
        sweep.run(lambda c: [x.wait() for x in token_copy(c)], between)
        loop(pairs - 1, settle)
        sweep.drain()

    dma = pltpu.SemaphoreType.DMA
    anyspec = pl.BlockSpec(memory_space=pl.ANY)
    S = jax.ShapeDtypeStruct
    return pl.pallas_call(
        kernel,
        in_specs=[anyspec] * 8,
        out_specs=[anyspec] * 2,
        out_shape=[S((D, FF), f32), S((FF, D), f32)],
        scratch_shapes=sweep_scratch(T, D, nb, tc) + [
            pltpu.VMEM((2 * per, D, rows), f32), pltpu.VMEM((2 * per, rows, D), f32),
            dma((2, nc)), dma((2, 2 * per)), dma((2, 2 * per))],
        compiler_params=pltpu.CompilerParams(vmem_limit_bytes=63 << 20),
        cost_estimate=pl.CostEstimate(flops=8 * nb * nblk * T * D, bytes_accessed=4 * T * D + 24 * FF * D, transcendentals=0),
        name="final",
    )


def solution(mesh):
    n_stage = mesh.shape["stage"]
    n_data = mesh.shape["data"]
    ny = int(round(n_data ** 0.5))
    nz = n_data // ny
    ns, nb, tc, sub, done = 128, 256, 1024, 256, 12
    when = (4, 7, 9, 15, 20)
    times = ((-99, -99, 0, 0, 0, 0, 0, 0, 0, 1, 1, 1), (0, 2, 2, 4, 4, 6, 8, 11, 14, 14, 17, 20), (0, 1, 1, 3, 3, 5, 7, 10, 12, 12, 15, 17), (0, 2, 2, 5, 5, 9, 12, 18, 21, 21, 26, 29))
    ahead = (30, 10, 12, 8)

    def local_step(x_in, y_tgt, w_up, w_down, gain):
        n_micro, T, D = x_in.shape
        FF = w_up.shape[2]
        w1, w2 = w_up[0], w_down[0]
        tok_total = n_data * n_micro * T
        n_pre = (FF - ns * n_data) // nb
        rg, dhg, _, wt2, ap, dg, loss = chain_call(T, D, FF, ny, nz, n_stage, tok_total, 256, 4, nb, tc, n_pre, times, ahead)(x_in, y_tgt, gain, w1, w2)
        rg = rg.reshape(tok_total, D)
        dhg = dhg.reshape(tok_total, D)
        ga, gb, lu, ld = spread_call(tok_total, D, FF, ny, nz, ns, nb, tc, sub, done, when)(rg, dhg, ap, w1, wt2)
        ga = ga.reshape(n_data, D, ns)
        gb = gb.reshape(n_data, ns, D)
        up, down = final_call(tok_total, D, FF, n_data, ns, nb, tc, sub, done)(rg, dhg, ap, wt2, ga, gb, lu, ld)
        return up[None], down[None], dg, loss[0, :1]

    return jax.shard_map(local_step, mesh=mesh, in_specs=(P(("part", "data"), None, None), P(("part", "data"), None, None), P("stage", None, None), P("stage", None, None), P("stage", None)), out_specs=(P(("part", "stage"), None, None), P(("part", "stage"), None, None), P(("part", "stage"), None), P("part")), check_vma=False)
```
